256 devices in a mesh: batch: 64 (over z, x, y_hi), chan: 4 (over y_lo, core).
Axes of the slice: x: 4, y: 4 (y_hi: 2, y_lo: 2; y = y_hi * 2 + y_lo), z: 8, core: 2. Of those that a mesh axis runs over, the one named last changes fastest.
Arguments:
- signal: float32 [1024, 32768], P('chan', 'batch'), may hold values from -6 to 6
- cotangent: float32 [1024, 32768], P('chan', 'batch'), may hold values from -6 to 6
- first_layer: float32 [33, 64], replicated, may hold values from -5 to 5
- second_layer: float32 [64, 1024], P(None, 'chan'), may hold values from -0.75 to 0.75
- decay_rate: float32 [1024], P('chan'), may hold values from 0.3 to 600
- skip_gain: float32 [1024], P('chan'), may hold values from -4 to 4
Outputs:
- input_grad: float32 [1024, 32768], P('chan', 'batch')
- first_grad: float32 [33, 64], replicated
- second_grad: float32 [64, 1024], P(None, 'chan')
- decay_grad: float32 [1024], P('chan')
- skip_grad: float32 [1024], P('chan')
The draws below stay inside these ranges and needn't reach their ends.
All inputs are finite; a program needn't handle non-finite values.
Results may differ from the reference program's by a relative error of at most 0.0003.
Values sent between devices are 32-bit elements; how exact they have to be, the bound alone decides.
A program may use at most 128 MiB of HBM per device.

```python
import math
import jax
import jax.numpy as jnp
from jax import lax

WIDTH = 1024
LENGTH = 32768
ORDER = 64
BANDS = 16
EMBED = 33


def block_levels(key, shape, pieces, smallest, top_value):
    gain, own = 1.0, jax.random.fold_in(key, 6)
    for position, parts in pieces:
        heights = jnp.exp(jax.random.uniform(jax.random.fold_in(own, position), (parts,), jnp.float32, smallest / len(pieces), top_value / len(pieces)))
        gain = gain * jnp.repeat(heights, shape[position] // parts).reshape([-1 if axis == position else 1 for axis in range(len(shape))])
    return gain


def scatter_about(own_key, extent, deviation, reach, split=(), kind=jnp.bfloat16):
    result = deviation * jax.random.normal(own_key, extent, jnp.float32)
    if split:
        result = result * block_levels(own_key, extent, split, -0.22, 0.18)
    return jnp.clip(result, -reach, reach).astype(kind)


def setup_inputs(seed: int = 0) -> dict:
    key_of = jax.random.split(jax.random.key(seed), 7)
    return {
        "signal": scatter_about(key_of[0], (WIDTH, LENGTH), 1.0, 6.0, ((0, 4), (1, 64)), jnp.float32),
        "cotangent": scatter_about(key_of[1], (WIDTH, LENGTH), 1.0, 6.0, ((0, 4), (1, 64)), jnp.float32),
        "first_layer": scatter_about(key_of[2], (EMBED, ORDER), 1.0, 5.0, (), jnp.float32),
        "second_layer": scatter_about(key_of[3], (ORDER, WIDTH), ORDER ** -0.5, 0.75, ((1, 4),), jnp.float32),
        "decay_rate": jnp.clip(jnp.exp(math.log(600.0) - 7.6009024 * jax.random.uniform(key_of[4], (WIDTH,), jnp.float32) ** block_levels(key_of[4], (WIDTH,), ((0, 4),), -0.2, 0.2)), 0.3, 600.0),
        "skip_gain": scatter_about(key_of[5], (WIDTH,), 1.0, 4.0, ((0, 4),), jnp.float32),
    }


precise = lax.Precision.HIGHEST
epsilon = 1e-06

def features(positions, length, band_count):
    band_index = jnp.arange(1, band_count + 1, dtype=jnp.int32)
    phase = (band_index[:, None] * positions[None, :] % length).astype(jnp.float32) * (2.0 * math.pi / length)
    linear = positions.astype(jnp.float32)[None, :] / length
    return jnp.concatenate([linear, jnp.cos(phase), jnp.sin(phase)], axis=0)

def reference(signal, cotangent, first_layer, second_layer, decay_rate, skip_gain):
    positions = jnp.arange(LENGTH, dtype=jnp.int32)
    embed = features(positions, LENGTH, BANDS)
    before = jnp.dot(first_layer.T, embed, precision=precise)
    basis = jnp.sin(before)
    fraction = positions.astype(jnp.float32) / LENGTH
    factor = 1.0 / math.sqrt(LENGTH)
    padded = 2 * LENGTH
    stride = 64
    blocks_count = WIDTH // stride

    def step(carry, index):
        start = (index * stride).astype(jnp.int32)
        values = lax.dynamic_slice_in_dim(signal, start, stride, 0)
        cotan = lax.dynamic_slice_in_dim(cotangent, start, stride, 0)
        columns = lax.dynamic_slice_in_dim(second_layer, start, stride, 1)
        rates = lax.dynamic_slice_in_dim(decay_rate, start, stride, 0)
        gains = lax.dynamic_slice_in_dim(skip_gain, start, stride, 0)
        window = jnp.exp(-rates[:, None] * fraction[None, :])
        shaped = window * jnp.dot(columns.T, basis, precision=precise)
        norms = jnp.sqrt(lax.optimization_barrier(jnp.sum(shaped * shaped, axis=1, keepdims=True)) + epsilon)
        filt = shaped / norms
        spec_val = jnp.fft.rfft(values, n=padded)
        spec_cot = jnp.fft.rfft(cotan, n=padded)
        spec_filt = jnp.fft.rfft(filt, n=padded)
        in_grad = jnp.fft.irfft(jnp.conj(spec_filt) * spec_cot, n=padded)[:, :LENGTH] + gains[:, None] * cotan
        dfilt = factor * jnp.fft.irfft(jnp.conj(spec_val) * spec_cot, n=padded)[:, :LENGTH]
        skip_part = factor * lax.optimization_barrier(jnp.sum(cotan * values, axis=1))
        project = lax.optimization_barrier(jnp.sum(filt * dfilt, axis=1, keepdims=True))
        draw = (dfilt - filt * project) / norms
        decay_part = -lax.optimization_barrier(jnp.sum(draw * shaped * fraction[None, :], axis=1))
        dmix = draw * window
        second_part = jnp.dot(basis, dmix.T, precision=precise)
        carry = carry + jnp.dot(columns, dmix, precision=precise)
        return (carry, (in_grad.astype(jnp.float32), second_part, decay_part, skip_part))
    dbasis, results = lax.scan(step, jnp.zeros((ORDER, LENGTH), jnp.float32), jnp.arange(blocks_count, dtype=jnp.int32))
    in_blocks, second_blocks, decay_blocks, skip_blocks = results
    input_grad = in_blocks.reshape(WIDTH, LENGTH)
    second_grad = jnp.transpose(second_blocks, (1, 0, 2)).reshape(ORDER, WIDTH)
    decay_grad = decay_blocks.reshape(WIDTH)
    skip_grad = skip_blocks.reshape(WIDTH)
    first_grad = jnp.dot(embed, (jnp.cos(before) * dbasis).T, precision=precise)
    return (input_grad, first_grad, second_grad, decay_grad, skip_grad)
```

```python
import functools
import math

import jax
import jax.numpy as jnp
import numpy as np
from jax import lax
from jax.experimental import pallas as pl
from jax.experimental.pallas import tpu as pltpu
from jax.sharding import PartitionSpec as P

GROUPS = 64
PEERS = 4
NARROW = 4
LENGTH = 32768
LOCAL = LENGTH // GROUPS
ORDER = 64
BANDS = 16
EMBED = 33
A = 128
M = 256
TERMS = 2 * BANDS + 2
FACTOR = 1.0 / math.sqrt(LENGTH)
EPSILON = 1e-06
F32 = jnp.float32
BF16 = jnp.bfloat16
MESH = pl.DeviceIdType.MESH
KK = 4


def split_np(x):
    hi = np.asarray(x, np.float32).astype(jnp.bfloat16)
    lo = (np.asarray(x, np.float64) - hi.astype(np.float64)).astype(jnp.bfloat16)
    return hi, lo


@functools.cache
def tables():
    row = np.arange(A)
    place = 2 * (row % 64) + row // 64
    k1 = np.arange(A)[:, None] + 0.25
    m = np.arange(M)
    phase = 2 * np.pi * k1 * place[None, :] / A
    first = np.concatenate([np.cos(phase), -np.sin(phase)], axis=0)
    twist = -2 * np.pi * k1 * m[None, :] / LENGTH
    grid = 2 * np.pi * (np.outer(m, m) % M) / M
    c, s = np.cos(grid), np.sin(grid)
    second = np.block([[c, -s], [s, c]])
    last = np.concatenate([np.cos(phase), -np.sin(phase)], axis=0).T / LENGTH
    out = {}
    out["t1h"], out["t1l"] = split_np(first)
    out["dh"], out["dl"] = split_np(second)
    out["eh"], out["el"] = split_np(second.T)
    out["t2h"], out["t2l"] = split_np(last)
    out["twr"] = np.cos(twist).astype(np.float32)
    out["twi"] = np.sin(twist).astype(np.float32)
    b = np.arange(1, BANDS + 1)
    alpha = 2 * np.pi * np.outer(place, b) / A
    beta = 2 * np.pi * np.outer(b, m) / LENGTH
    ones = np.ones((A, 1))
    ca = np.concatenate([np.cos(alpha), np.cos(alpha), place[:, None] / A, ones], axis=1)
    sa = np.concatenate([np.sin(alpha), np.sin(alpha), 0 * ones, 0 * ones], axis=1)
    q = np.concatenate([np.cos(beta), np.sin(beta), np.ones((1, M)), m[None, :] / LENGTH], axis=0)
    wide = lambda x: np.pad(np.tile(x, (1, 6)), ((0, 0), (0, 256 - 6 * TERMS))).astype(np.float32)
    out["ca"], out["sa"] = wide(ca), wide(sa)
    qh, rest = split_np(q)[0], None
    qm = (q - qh.astype(np.float64)).astype(jnp.bfloat16)
    ql = (q - qh.astype(np.float64) - qm.astype(np.float64)).astype(jnp.bfloat16)
    q6 = np.concatenate([qh, qm, ql, qh, qm, qh], axis=0)
    out["q6"] = np.pad(q6, ((0, 256 - 6 * TERMS), (0, 0)))
    qb = np.zeros((2 * M, 128), jnp.bfloat16)
    qb[:M, :TERMS] = qh.T
    qb[:M, TERMS : 2 * TERMS] = qm.T
    qb[M:, :TERMS] = qh.T
    out["qb"] = qb
    e1 = np.zeros((128, 64), np.float32)
    e2 = np.zeros((128, 64), np.float32)
    for copy in range(2):
        o = copy * TERMS
        for i in range(BANDS):
            e1[o + i, 1 + i] = 1
            e1[o + BANDS + i, 1 + BANDS + i] = 1
            e2[o + i, 1 + BANDS + i] = 1
            e2[o + BANDS + i, 1 + i] = -1
        e1[o + 2 * BANDS, 0] = 1
        e1[o + 2 * BANDS + 1, 0] = 1
    zero = np.zeros_like(e1)
    out["ea"] = np.concatenate([np.concatenate([e1, zero], 1), np.concatenate([zero, e1], 1)], 0)
    out["eb"] = np.concatenate([np.concatenate([e2, zero], 1), np.concatenate([zero, e2], 1)], 0)
    return out


NAMES = ("t1h", "t1l", "dh", "dl", "eh", "el", "t2h", "t2l", "twr", "twi", "ca", "sa", "q6", "qb", "ea", "eb")


def halves(x):
    hi = x.astype(BF16)
    return hi, (x - hi.astype(F32)).astype(BF16)


def dot(a, b):
    return jnp.dot(a, b, preferred_element_type=F32)


def mm3(ah, al, bh, bl):
    return dot(ah, bh) + dot(al, bh) + dot(ah, bl)


def sin_cos(x):
    magic = 12582912.0
    turns = (x * (0.5 / math.pi) + magic) - magic
    h = x * 0.5 - turns * 3.140625
    h = h - turns * 9.67502593994140625e-4
    h = h - turns * 1.509957990978376e-07
    z = h * h
    s = 2.59701174e-06
    s = s * z - 1.98052345e-04
    s = s * z + 8.33299813e-03
    s = s * z - 1.66666563e-01
    s = h + h * (z * s)
    c = -2.61670784e-07
    c = c * z + 2.47680152e-05
    c = c * z - 1.38885497e-03
    c = c * z + 4.16666549e-02
    c = c * z - 0.5
    c = c * z + 1.0
    twice = s + s
    return twice * c, 1.0 - twice * s


def kernel(comm, *refs):
    it = iter(refs)
    sig, cot, u_ref, v_ref, cols, scal = (next(it) for _ in range(6))
    t = {name: next(it) for name in NAMES}
    out, gath_out, first_out = (next(it) for _ in range(3))
    (s_send, c_send, s_recv, c_recv, y_send, y_recv) = (next(it) for _ in range(6))
    (basis, cosb, pbuf, bbuf, raw, dmix) = (next(it) for _ in range(6))
    (xh, xl, gh, gl, spec_f, spec_c, spec_s, wbuf) = (next(it) for _ in range(8))
    (mid, gath, sgs, ug, vg, red_a, red_b, red_c) = (next(it) for _ in range(8))
    (send_sem, recv_sem) = (next(it) for _ in range(2))

    if comm:
        bi = lax.axis_index("batch")
        ci = lax.axis_index("chan")
        barrier = pltpu.get_barrier_semaphore()

        def greet(i, _):
            pl.semaphore_signal(barrier, inc=1, device_id={"batch": lax.rem(bi + i, GROUPS)}, device_id_type=MESH)
            return 0

        lax.fori_loop(1, GROUPS, greet, 0)
        for i in range(1, PEERS):
            pl.semaphore_signal(barrier, inc=1, device_id={"chan": lax.rem(ci + i, PEERS)}, device_id_type=MESH)

    def spread(src, dst, slot, rows):
        mine = pl.ds(pl.multiple_of(bi * rows, rows), rows)

        def push(i, _):
            p = lax.rem(bi + i, GROUPS)
            pltpu.make_async_remote_copy(
                src_ref=src.at[pl.ds(pl.multiple_of(p * rows, rows), rows)],
                dst_ref=dst.at[mine],
                send_sem=send_sem.at[slot],
                recv_sem=recv_sem.at[slot],
                device_id={"batch": p},
                device_id_type=MESH,
            ).start()
            return 0

        lax.fori_loop(1, GROUPS, push, 0)
        dst[mine, :] = src[mine, :]

    def landed(dst, sem, slot, rows):
        part = dst.at[pl.ds(0, (GROUPS - 1) * rows)]
        pltpu.make_async_copy(part, part, sem.at[slot]).wait()

    if comm:
        for q in range(4):
            lanes = slice(q * 128, q * 128 + 128)
            c_send[pl.ds(q, 256, stride=4), :] = cot[:, lanes]
            s_send[pl.ds(q, 256, stride=4), :] = sig[:, lanes]
        pl.semaphore_wait(barrier, GROUPS - 1 + PEERS - 1)
        spread(c_send, c_recv, 0, 16)
        spread(s_send, s_recv, 1, 16)
    else:
        c_recv[...] = cot[...]
        s_recv[...] = sig[...]

    lane = lax.broadcasted_iota(jnp.int32, (1, 256), 1)
    raw[...] = jnp.zeros_like(raw)

    def hidden(step, _):
        for i in range(KK):
            k = step * KK + i
            for r in range(0, A, 32):
                rows = slice(r, r + 32)
                p = u_ref[pl.ds(k, 1), :] * t["ca"][rows, :] + v_ref[pl.ds(k, 1), :] * t["sa"][rows, :]
                hi = p.astype(BF16).astype(F32)
                rest = p - hi
                med = rest.astype(BF16).astype(F32)
                low = rest - med
                p = jnp.where(lane < 3 * TERMS, hi, jnp.where(lane < 5 * TERMS, med, low))
                pbuf[i * A + r : i * A + r + 32, :] = p.astype(BF16)
        bbuf[...] = dot(pbuf[...], t["q6"][...])

        for r in range(0, A, 16):
            rows = slice(r, r + 16)
            acc = [raw[c, rows, :] for c in range(NARROW)]
            for i in range(KK):
                k = step * KK + i
                sine, cosine = sin_cos(bbuf[i * A + r : i * A + r + 16, :])
                basis[k, rows, :] = sine
                cosb[k, rows, :] = cosine
                for c in range(NARROW):
                    acc[c] = acc[c] + sine * cols[k, c]
            for c in range(NARROW):
                raw[c, rows, :] = acc[c]
        return 0

    lax.fori_loop(0, ORDER // KK, hidden, 0)

    row = lax.broadcasted_iota(jnp.int32, (A, M), 0)
    col = lax.broadcasted_iota(jnp.int32, (A, M), 1)
    place = 512 * lax.rem(row, 64) + 256 * (row // 64) + col
    fraction = place.astype(F32) * (1.0 / LENGTH)

    def total(x):
        return jnp.sum(jnp.sum(x, axis=1, keepdims=True), axis=0, keepdims=True)

    def forward(load, spec):
        for c in range(NARROW):
            xh[...], xl[...] = halves(load(c))
            f = mm3(t["t1h"][...], t["t1l"][...], xh[...], xl[...])
            re, im = f[:A], f[A:]
            rows = slice(c * A, c * A + A)
            gh[rows, :M], gl[rows, :M] = halves(re * t["twr"][...] - im * t["twi"][...])
            gh[rows, M:], gl[rows, M:] = halves(re * t["twi"][...] + im * t["twr"][...])
        spec[...] = mm3(gh[...], gl[...], t["dh"][...], t["dl"][...])

    def inverse(one, two, store):
        for c in range(NARROW):
            rows = slice(c * A, c * A + A)
            r1, i1, r2, i2 = one[rows, :M], one[rows, M:], two[rows, :M], two[rows, M:]
            gh[rows, :M], gl[rows, :M] = halves(r1 * r2 + i1 * i2)
            gh[rows, M:], gl[rows, M:] = halves(r1 * i2 - i1 * r2)
        wbuf[...] = mm3(gh[...], gl[...], t["eh"][...], t["el"][...])
        for c in range(NARROW):
            rows = slice(c * A, c * A + A)
            re, im = wbuf[rows, :M], wbuf[rows, M:]
            mid[:A, :] = re * t["twr"][...] + im * t["twi"][...]
            mid[A:, :] = im * t["twr"][...] - re * t["twi"][...]
            h, low = halves(mid[...])
            store(c, mm3(t["t2h"][...], t["t2l"][...], h, low))

    def blocks_of(buf, c):
        parts = [
            [buf[pl.ds(4 * c + 2 * h + q, 64, stride=16), :] for q in range(2)] for h in range(2)
        ]
        return jnp.concatenate([jnp.concatenate(p, axis=1) for p in parts], axis=0)

    norms = []
    for c in range(NARROW):
        value = raw[c] * jnp.exp(-scal[0, c] * fraction)
        raw[c] = value
        norms.append(jnp.sqrt(total(value * value) + EPSILON))
    forward(lambda c: raw[c] / norms[c], spec_f)

    if comm:
        landed(c_recv, recv_sem, 0, 16)
    forward(lambda c: blocks_of(c_recv, c), spec_c)

    def store_grad(c, y):
        y = y + scal[1, c] * blocks_of(c_recv, c)
        for h in range(2):
            for q in range(2):
                y_send[pl.ds(4 * c + 2 * h + q, 64, stride=16), :] = y[h * 64 : h * 64 + 64, q * 128 : q * 128 + 128]

    inverse(spec_f, spec_c, store_grad)
    if comm:
        spread(y_send, y_recv, 2, 16)
        landed(s_recv, recv_sem, 1, 16)
    forward(lambda c: blocks_of(s_recv, c), spec_s)
    sgs[...] = jnp.zeros_like(sgs)

    def store_filter(c, y):
        dfilt = FACTOR * y
        norm = norms[c]
        value = raw[c]
        filt = value / norm
        project = total(filt * dfilt)
        draw = (dfilt - filt * project) / norm
        decay = -jnp.sum(draw * value * fraction, axis=0, keepdims=True)
        skip = FACTOR * jnp.sum(blocks_of(c_recv, c) * blocks_of(s_recv, c), axis=0, keepdims=True)
        sgs[c * 128 + 64 : c * 128 + 65, :] = decay[:, :128] + decay[:, 128:]
        sgs[c * 128 + 65 : c * 128 + 66, :] = skip[:, :128] + skip[:, 128:]
        dmix[c] = draw * jnp.exp(-scal[0, c] * fraction)

    inverse(spec_s, spec_c, store_filter)

    def hidden_back(step, _):
        sums = [[jnp.zeros((8, 128), F32) for _ in range(NARROW)] for _ in range(KK)]
        for r in range(0, A, 16):
            rows = slice(r, r + 16)
            d = [dmix[c, rows, :] for c in range(NARROW)]
            for i in range(KK):
                k = step * KK + i
                b = basis[k, rows, :]
                g = d[0] * cols[k, 0]
                for c in range(1, NARROW):
                    g = g + d[c] * cols[k, c]
                g = g * cosb[k, rows, :]
                ghi, glo = halves(g)
                gh[i * A + r : i * A + r + 16, :M] = ghi
                gh[i * A + r : i * A + r + 16, M:] = glo
                for c in range(NARROW):
                    e = b * d[c]
                    sums[i][c] = sums[i][c] + ((e[:8, :128] + e[:8, 128:]) + (e[8:, :128] + e[8:, 128:]))
        for i in range(KK):
            for c in range(NARROW):
                sgs[pl.ds(c * 128 + step * KK + i, 1), :] = jnp.sum(sums[i][c], axis=0, keepdims=True)
        hmat = dot(gh[...], t["qb"][...])
        for i in range(KK):
            part = hmat[i * A : i * A + A]
            ug[pl.ds(step * KK + i, 1), :] = jnp.sum(part * t["ca"][:, :128], axis=0, keepdims=True)
            vg[pl.ds(step * KK + i, 1), :] = jnp.sum(part * t["sa"][:, :128], axis=0, keepdims=True)
        return 0

    lax.fori_loop(0, ORDER // KK, hidden_back, 0)

    high = lax.Precision.HIGHEST
    hdot = lambda a, b: jnp.dot(a, b, precision=high, preferred_element_type=F32)
    first = (
        hdot(ug[:32, :], t["ea"][:128, :])
        + hdot(ug[32:, :], t["ea"][128:, :])
        + hdot(vg[:32, :], t["eb"][:128, :])
        + hdot(vg[32:, :], t["eb"][128:, :])
    )
    ones = jnp.ones((8, 128), F32)
    sums = [
        lax.dot_general(
            ones, sgs[c * 128 : c * 128 + 128, :], (((1,), (1,)), ((), ())), precision=high, preferred_element_type=F32
        )[:1]
        for c in range(NARROW)
    ]
    block = jnp.concatenate(sums, axis=0)

    if not comm:
        for q in range(4):
            out[:, q * 128 : q * 128 + 128] = y_send[pl.ds(q, 256, stride=4), :]
        gath_out[...] = jnp.zeros_like(gath_out)
        gath_out[0] = block
        first_out[...] = first
        return

    gath[pl.ds(bi, 1)] = block[None]

    def tell(i, _):
        pltpu.make_async_remote_copy(
            src_ref=gath.at[bi],
            dst_ref=gath.at[bi],
            send_sem=send_sem.at[3],
            recv_sem=recv_sem.at[3],
            device_id={"batch": lax.rem(bi + i, GROUPS)},
            device_id_type=MESH,
        ).start()
        return 0

    def stage(buf, slot, value, me, count, target):
        buf[pl.ds(me, 1)] = value[None]
        for i in range(1, count):
            pltpu.make_async_remote_copy(
                src_ref=buf.at[me],
                dst_ref=buf.at[me],
                send_sem=send_sem.at[slot],
                recv_sem=recv_sem.at[slot],
                device_id=target(lax.rem(me + i, count)),
                device_id_type=MESH,
            ).start()
        if slot == 4:
            lax.fori_loop(1, GROUPS, tell, 0)
        part = buf.at[pl.ds(0, count - 1)]
        pltpu.make_async_copy(part, part, recv_sem.at[slot]).wait()
        pltpu.make_async_copy(part, part, send_sem.at[slot]).wait()
        value = buf[0]
        for i in range(1, count):
            value = value + buf[i]
        return value

    zi, xy = bi // 8, lax.rem(bi, 8)
    first = stage(red_a, 4, first, ci, PEERS, lambda p: {"chan": p})
    first = stage(red_b, 5, first, zi, 8, lambda p: {"batch": p * 8 + xy})
    first = stage(red_c, 6, first, xy, 8, lambda p: {"batch": zi * 8 + p})
    first_out[...] = first

    landed(y_recv, recv_sem, 2, 16)
    for q in range(4):
        out[:, q * 128 : q * 128 + 128] = y_recv[pl.ds(q, 256, stride=4), :]
    landed(gath, recv_sem, 3, 1)
    gath_out[...] = gath[...]
    landed(c_send, send_sem, 0, 16)
    landed(s_send, send_sem, 1, 16)
    landed(y_send, send_sem, 2, 16)
    landed(gath, send_sem, 3, 1)


def call(comm, sig, cot, u, v, cols, scal):
    vmem = pl.BlockSpec(memory_space=pltpu.VMEM)
    smem = pl.BlockSpec(memory_space=pltpu.SMEM)
    t = tables()
    rows = GROUPS * 16
    line = lambda: pltpu.VMEM((rows, 128), F32)
    scratch = [line() for _ in range(6)]
    scratch += [
        pltpu.VMEM((ORDER, A, M), F32),
        pltpu.VMEM((ORDER, A, M), F32),
        pltpu.VMEM((KK * A, 256), BF16),
        pltpu.VMEM((KK * A, M), F32),
        pltpu.VMEM((NARROW, A, M), F32),
        pltpu.VMEM((NARROW, A, M), F32),
        pltpu.VMEM((A, M), BF16),
        pltpu.VMEM((A, M), BF16),
        pltpu.VMEM((NARROW * A, 2 * M), BF16),
        pltpu.VMEM((NARROW * A, 2 * M), BF16),
        pltpu.VMEM((NARROW * A, 2 * M), F32),
        pltpu.VMEM((NARROW * A, 2 * M), F32),
        pltpu.VMEM((NARROW * A, 2 * M), F32),
        pltpu.VMEM((NARROW * A, 2 * M), F32),
        pltpu.VMEM((2 * A, M), F32),
        pltpu.VMEM((GROUPS, NARROW, 128), F32),
        pltpu.VMEM((NARROW * 128, 128), F32),
        pltpu.VMEM((ORDER, 128), F32),
        pltpu.VMEM((ORDER, 128), F32),
        pltpu.VMEM((PEERS, 32, 128), F32),
        pltpu.VMEM((8, 32, 128), F32),
        pltpu.VMEM((8, 32, 128), F32),
        pltpu.SemaphoreType.DMA((7,)),
        pltpu.SemaphoreType.DMA((7,)),
    ]
    params = dict(vmem_limit_bytes=56 * 2**20)
    if comm:
        params.update(collective_id=0, has_side_effects=True)
    return pl.pallas_call(
        functools.partial(kernel, comm),
        out_shape=(
            jax.ShapeDtypeStruct((256, LOCAL), F32),
            jax.ShapeDtypeStruct((GROUPS, NARROW, 128), F32),
            jax.ShapeDtypeStruct((32, 128), F32),
        ),
        in_specs=[vmem] * 4 + [smem] * 2 + [vmem] * len(NAMES),
        out_specs=(vmem, vmem, vmem),
        scratch_shapes=scratch,
        compiler_params=pltpu.CompilerParams(**params),
        name="hyena_back",
    )(sig, cot, u, v, cols, scal, *[jnp.asarray(t[name]) for name in NAMES])


def terms(first_layer):
    linear = first_layer[:1]
    cosine, sine = first_layer[1 : 1 + BANDS], first_layer[1 + BANDS :]
    u = jnp.concatenate([cosine, sine, linear, linear], axis=0).T
    v = jnp.concatenate([sine, -cosine, 0 * linear, 0 * linear], axis=0).T
    wide = lambda x: jnp.pad(jnp.tile(x, (1, 6)), ((0, 0), (0, 256 - 6 * TERMS)))
    return wide(u), wide(v)


def local(signal, cotangent, first_layer, second_layer, decay_rate, skip_gain):
    start = lax.axis_index("batch") * NARROW
    u, v = terms(first_layer)
    cols = lax.dynamic_slice_in_dim(second_layer, start, NARROW, 1)
    scal = jnp.stack([lax.dynamic_slice_in_dim(x, start, NARROW, 0) for x in (decay_rate, skip_gain)])
    grad, gath, first = call(True, signal, cotangent, u, v, cols, scal)
    gath = gath.reshape(GROUPS * NARROW, 128)
    first_grad = jnp.concatenate([first[:, :EMBED], first[:, 64 : 64 + EMBED]], axis=0).T
    return grad, first_grad, gath[:, :ORDER].T, gath[:, ORDER], gath[:, ORDER + 1]


def solution(mesh):
    placed = (P("chan", "batch"), P("chan", "batch"), P(), P(None, "chan"), P("chan"), P("chan"))
    return jax.shard_map(
        local,
        mesh=mesh,
        in_specs=placed,
        out_specs=(P("chan", "batch"), P(), P(None, "chan"), P("chan"), P("chan")),
        check_vma=False,
    )
```

```python
import functools
import math

import jax
import jax.numpy as jnp
import numpy as np
from jax import lax
from jax.experimental import pallas as pl
from jax.experimental.pallas import tpu as pltpu
from jax.sharding import PartitionSpec as P

GROUPS = 64
PEERS = 4
NARROW = 4
LENGTH = 32768
LOCAL = LENGTH // GROUPS
ORDER = 64
BANDS = 16
EMBED = 33
A = 128
M = 256
TERMS = 2 * BANDS + 2
FACTOR = 1.0 / math.sqrt(LENGTH)
EPSILON = 1e-06
F32 = jnp.float32
BF16 = jnp.bfloat16
MESH = pl.DeviceIdType.MESH
SIN = (6.283185158626588, -10.33541366421067, 5.100061181598971, -1.19608076409451, 0.154421099195309)
COS = (0.9999999530044438, -4.934792784653484, 4.058410137182749, -1.331866894431586, 0.21966648431395203)
KK = 4
EARLY = 4
VMEM_LIMIT = 60 * 2**20


def split_np(x):
    hi = np.asarray(x, np.float32).astype(jnp.bfloat16)
    lo = (np.asarray(x, np.float64) - hi.astype(np.float64)).astype(jnp.bfloat16)
    return hi, lo


@functools.cache
def tables():
    row = np.arange(A)
    place = 2 * (row % 64) + row // 64
    k1 = np.arange(A)[:, None] + 0.25
    m = np.arange(M)
    phase = 2 * np.pi * k1 * place[None, :] / A
    first = np.concatenate([np.cos(phase), -np.sin(phase)], axis=0)
    twist = -2 * np.pi * k1 * m[None, :] / LENGTH
    grid = 2 * np.pi * (np.outer(m, m) % M) / M
    c, s = np.cos(grid), np.sin(grid)
    second = np.block([[c, -s], [s, c]])
    last = np.concatenate([np.cos(phase), -np.sin(phase)], axis=0).T / LENGTH
    out = {}
    out["t1h"], out["t1l"] = split_np(first)
    out["dh"], out["dl"] = split_np(second)
    out["t2h"], out["t2l"] = split_np(last)
    out["twr"] = np.cos(twist).astype(np.float32)
    out["twi"] = np.sin(twist).astype(np.float32)
    b = np.arange(1, BANDS + 1)
    alpha = 2 * np.pi * np.outer(place, b) / A
    beta = 2 * np.pi * np.outer(b, m) / LENGTH
    ones = np.ones((A, 1))
    ca = np.concatenate([np.cos(alpha), np.cos(alpha), place[:, None] / A, ones], axis=1)
    sa = np.concatenate([np.sin(alpha), np.sin(alpha), 0 * ones, 0 * ones], axis=1)
    q = np.concatenate([np.cos(beta), np.sin(beta), np.ones((1, M)), m[None, :] / LENGTH], axis=0)
    wide = lambda x: np.pad(np.tile(x, (1, 3)), ((0, 0), (0, 128 - 3 * TERMS))).astype(np.float32)
    out["ca"], out["sa"] = wide(ca), wide(sa)
    qh, rest = split_np(q)[0], None
    qm = (q - qh.astype(np.float64)).astype(jnp.bfloat16)
    out["q3"] = np.pad(np.concatenate([qh, qm, qh], axis=0), ((0, 128 - 3 * TERMS), (0, 0)))
    qb = np.zeros((2 * M, 128), jnp.bfloat16)
    qb[:M, :TERMS] = qh.T
    qb[:M, TERMS : 2 * TERMS] = qm.T
    qb[M:, :TERMS] = qh.T
    out["qb"] = qb
    e1 = np.zeros((TERMS, 40), np.float32)
    e2 = np.zeros((TERMS, 40), np.float32)
    for i in range(BANDS):
        e1[i, 1 + i] = 1
        e1[BANDS + i, 1 + BANDS + i] = 1
        e2[i, 1 + BANDS + i] = 1
        e2[BANDS + i, 1 + i] = -1
    e1[2 * BANDS :, 0] = 1
    out["ea"], out["eb"] = wide(e1.T), wide(e2.T)
    return out


NAMES = ("t1h", "t1l", "dh", "dl", "t2h", "t2l", "twr", "twi", "ca", "sa", "q3", "qb", "ea", "eb")


def halves(x):
    hi = x.astype(BF16)
    return hi, (x - hi.astype(F32)).astype(BF16)


def dot(a, b):
    return jnp.dot(a, b, preferred_element_type=F32)


def mm3(ah, al, bh, bl):
    return dot(ah, bh) + dot(al, bh) + dot(ah, bl)


def sin_cos(x):
    magic = 12582912.0
    f = x - ((x + magic) - magic)
    z = f * f
    s = SIN[4]
    for a in SIN[3::-1]:
        s = s * z + a
    s = s * f
    c = COS[4]
    for a in COS[3::-1]:
        c = c * z + a
    return s * c, 1.0 - (0.5 * s) * s


def kernel(comm, *refs):
    it = iter(refs)
    take = lambda n: [next(it) for _ in range(n)]
    sig_in, cot_in, first_in, second_in, rate_in, gain_in = take(6)
    t_in = dict(zip(NAMES, take(len(NAMES))))
    y_recv, gath, first_out = take(3)
    t = dict(zip(NAMES, take(len(NAMES))))
    sig, cot, weights, cols, rate, gain = take(6)
    s_send, c_send = take(2)
    s_recv, c_recv, y_send = take(2), next(it), next(it)
    basis, cosb, part, pbuf, bbuf, raw, dmix = take(7)
    xh, xl, gh, gl, spec_f, spec_c, spec_s, wbuf = take(8)
    mid, sgs, u_ref, v_ref, ug, vg, red_a, red_b, red_c = take(9)
    send_sem, recv_sem, load_sem = take(3)

    bi = lax.axis_index("batch") if comm else 0
    ci = lax.axis_index("chan") if comm else 0
    peer = lambda i: lax.rem(bi + 1 + lax.rem(i + 31, GROUPS - 1), GROUPS)
    loads = [(cot_in, cot), (sig_in, sig), (first_in, weights), (second_in, cols), (rate_in, rate), (gain_in, gain)]
    loads += [(t_in[name], t[name]) for name in NAMES]
    loads = [pltpu.make_async_copy(src, dst, load_sem.at[i]) for i, (src, dst) in enumerate(loads)]
    for load in loads[:2]:
        load.start()

    if comm:
        barrier = pltpu.get_barrier_semaphore()

        def greet(i, _):
            pl.semaphore_signal(barrier, inc=1, device_id={"batch": peer(i)}, device_id_type=MESH)
            return 0

        lax.fori_loop(0, GROUPS - 1, greet, 0)
        for i in range(1, PEERS):
            pl.semaphore_signal(barrier, inc=1, device_id={"chan": lax.rem(ci + i, PEERS)}, device_id_type=MESH)

    for load in loads[2:]:
        load.start()

    def spread(src, dst, slot, skip, step, at, to, rows=8):
        def push(i, _):
            p = peer(i)
            pltpu.make_async_remote_copy(
                src_ref=src.at[pl.ds(pl.multiple_of(p * skip + at, 8), rows)],
                dst_ref=dst.at[pl.ds(pl.multiple_of(bi * step + to, 8), rows)],
                send_sem=send_sem.at[slot],
                recv_sem=recv_sem.at[slot],
                device_id={"batch": p},
                device_id_type=MESH,
            ).start()
            return 0

        lax.fori_loop(0, GROUPS - 1, push, 0)
        own = pl.ds(pl.multiple_of(bi * step + to, 8), rows)
        dst[own, :] = src[pl.ds(pl.multiple_of(bi * skip + at, 8), rows), :]

    def landed(span, sem, slot):
        pltpu.make_async_copy(span, span, sem.at[slot]).wait()

    def arrived(buf, sem, slot):
        landed(buf.at[pl.ds(0, (GROUPS - 1) * 8)], sem, slot)

    for q in range(4 if comm else 0):
        if q == 0:
            loads[0].wait()
        c_send[pl.ds(q, 256, stride=4), :] = cot[:, q * 128 : q * 128 + 128]
    for q in range(4 if comm else 0):
        if q == 0:
            loads[1].wait()
        s_send[pl.ds(q, 256, stride=4), :] = sig[:, q * 128 : q * 128 + 128]
    if not comm:
        loads[0].wait()
        loads[1].wait()
        for h in range(2):
            for r in range(4):
                rows = pl.ds(h * 512 + r * 128, 128)
                c_recv[h * 512 + r * 128 : h * 512 + r * 128 + 128, :] = cot[rows, :]
                s_recv[h][r * 128 : r * 128 + 128, :] = sig[rows, :]
    for load in loads[2:]:
        load.wait()

    high = lax.Precision.HIGHEST
    place = bi * NARROW
    turn = (((0,), (0,)), ((), ()))
    turns = 0.5 / math.pi
    u_ref[...] = turns * lax.dot_general(weights[...], t["ea"][:EMBED], turn, precision=high, preferred_element_type=F32)
    v_ref[...] = turns * lax.dot_general(weights[...], t["eb"][:EMBED], turn, precision=high, preferred_element_type=F32)

    lane = lax.broadcasted_iota(jnp.int32, (1, 128), 1)
    raw[...] = jnp.zeros_like(raw)

    def hidden(step, _):
        for i in range(KK):
            k = step * KK + i
            for r in range(0, A, 32):
                rows = slice(r, r + 32)
                p = u_ref[pl.ds(k, 1), :] * t["ca"][rows, :] + v_ref[pl.ds(k, 1), :] * t["sa"][rows, :]
                p = jnp.where(lane < 2 * TERMS, p, p - p.astype(BF16).astype(F32))
                pbuf[i * A + r : i * A + r + 32, :] = p.astype(BF16)
        bbuf[...] = dot(pbuf[...], t["q3"][...])

        for r in range(0, A, 16):
            rows = slice(r, r + 16)
            acc = [raw[c, rows, :] for c in range(NARROW)]
            for i in range(KK):
                k = step * KK + i
                sine, cosine = sin_cos(bbuf[i * A + r : i * A + r + 16, :])
                basis[k, rows, :] = sine
                cosb[k, rows, :] = cosine
                for c in range(NARROW):
                    acc[c] = acc[c] + sine * cols[k, place + c]
            for c in range(NARROW):
                raw[c, rows, :] = acc[c]
        return 0

    lax.fori_loop(0, EARLY, hidden, 0)
    if comm:
        pl.semaphore_wait(barrier, GROUPS - 1 + PEERS - 1)
        spread(c_send, c_recv, 0, 16, 16, 0, 0, 16)
        for h in range(2):
            spread(s_send, s_recv[h], 2 + h, 16, 8, 8 * h, 0)
    lax.fori_loop(EARLY, ORDER // KK, hidden, 0)

    row = lax.broadcasted_iota(jnp.int32, (A, M), 0)
    col = lax.broadcasted_iota(jnp.int32, (A, M), 1)
    where = 512 * lax.rem(row, 64) + 256 * (row // 64) + col
    fraction = where.astype(F32) * (1.0 / LENGTH)

    def total(x):
        return jnp.sum(jnp.sum(x, axis=1, keepdims=True), axis=0, keepdims=True)

    def forward(load, spec, at, count):
        for c in range(count):
            xh[...], xl[...] = halves(load(c))
            f = mm3(t["t1h"][...], t["t1l"][...], xh[...], xl[...])
            re, im = f[:A], f[A:]
            rows = slice(c * A, c * A + A)
            gh[rows, :M], gl[rows, :M] = halves(re * t["twr"][...] - im * t["twi"][...])
            gh[rows, M:], gl[rows, M:] = halves(re * t["twi"][...] + im * t["twr"][...])
        rows = slice(0, count * A)
        spec[at * A : (at + count) * A, :] = mm3(gh[rows, :], gl[rows, :], t["dh"][...], t["dl"][...])

    def inverse(one, at, pair, store):
        for c in range(2):
            rows = slice(c * A, c * A + A)
            from_one = slice((at + c) * A, (at + c + 1) * A)
            from_two = slice((2 * pair + c) * A, (2 * pair + c + 1) * A)
            r1, i1 = one[from_one, :M], one[from_one, M:]
            r2, i2 = spec_c[from_two, :M], spec_c[from_two, M:]
            gh[rows, :M], gl[rows, :M] = halves(r1 * r2 + i1 * i2)
            gh[rows, M:], gl[rows, M:] = halves(r1 * i2 - i1 * r2)
        rows = slice(0, 2 * A)
        across = (((1,), (1,)), ((), ()))
        tdot = lambda a, b: lax.dot_general(a, b, across, preferred_element_type=F32)
        high_part, low_part = gh[rows, :], gl[rows, :]
        wbuf[...] = (
            tdot(high_part, t["dh"][...]) + tdot(low_part, t["dh"][...]) + tdot(high_part, t["dl"][...])
        )
        for c in range(2):
            rows = slice(c * A, c * A + A)
            re, im = wbuf[rows, :M], wbuf[rows, M:]
            mid[:A, :] = re * t["twr"][...] + im * t["twi"][...]
            mid[A:, :] = im * t["twr"][...] - re * t["twi"][...]
            h, low = halves(mid[...])
            store(c, mm3(t["t2h"][...], t["t2l"][...], h, low))

    def blocks_of(buf, c, stride):
        parts = [[buf[pl.ds(4 * c + 2 * h + q, 64, stride=stride), :] for q in range(2)] for h in range(2)]
        return jnp.concatenate([jnp.concatenate(p, axis=1) for p in parts], axis=0)

    norms = []
    for c in range(NARROW):
        value = raw[c] * jnp.exp(-rate[place + c] * fraction)
        raw[c] = value
        norms.append(jnp.sqrt(total(value * value) + EPSILON))
    forward(lambda c: raw[c] / norms[c], spec_f, 0, NARROW)
    sgs[...] = jnp.zeros_like(sgs)

    def store_grad(c, y):
        y = y + gain[place + c] * blocks_of(c_recv, c, 16)
        for h in range(2):
            for q in range(2):
                y_send[pl.ds(4 * c + 2 * h + q, 64, stride=16), :] = y[h * 64 : h * 64 + 64, q * 128 : q * 128 + 128]

    if comm:
        landed(c_recv.at[pl.ds(0, (GROUPS - 1) * 16)], recv_sem, 0)
    forward(lambda c: blocks_of(c_recv, c, 16), spec_c, 0, NARROW)
    for pair in range(2):
        inverse(spec_f, 2 * pair, pair, lambda c, y: store_grad(2 * pair + c, y))
    if comm:
        spread(y_send, y_recv, 4, 16, 16, 0, 0, 16)
    else:
        for r in range(8):
            y_recv[r * 128 : r * 128 + 128, :] = y_send[r * 128 : r * 128 + 128, :]

    def filter_grad(pair):
        if comm:
            arrived(s_recv[pair], recv_sem, 2 + pair)
        forward(lambda c: blocks_of(s_recv[pair], c, 8), spec_s, 0, 2)

        def store(c, y):
            ch = 2 * pair + c
            dfilt = FACTOR * y
            norm = norms[ch]
            value = raw[ch]
            filt = value / norm
            project = total(filt * dfilt)
            draw = (dfilt - filt * project) / norm
            decay = -jnp.sum(draw * value * fraction, axis=0, keepdims=True)
            skip = blocks_of(c_recv, ch, 16) * blocks_of(s_recv[pair], c, 8)
            skip = FACTOR * jnp.sum(skip, axis=0, keepdims=True)
            sgs[ch * 128 + 64 : ch * 128 + 65, :] = decay[:, :128] + decay[:, 128:]
            sgs[ch * 128 + 65 : ch * 128 + 66, :] = skip[:, :128] + skip[:, 128:]
            dmix[ch] = draw * jnp.exp(-rate[place + ch] * fraction)

        inverse(spec_s, 0, pair, store)

    def half_back(step, _):
        for r in range(0, A, 16):
            rows = slice(r, r + 16)
            d = [dmix[c, rows, :] for c in range(2)]
            for i in range(KK):
                k = step * KK + i
                part[k, rows, :] = d[0] * cols[k, place] + d[1] * cols[k, place + 1]
        return 0

    def fill(buf, step):
        for r in range(0, A, 16):
            rows = slice(r, r + 16)
            d = [dmix[c, rows, :] for c in range(2, 4)]
            for i in range(KK):
                k = step * KK + i
                g = part[k, rows, :] + d[0] * cols[k, place + 2] + d[1] * cols[k, place + 3]
                ghi, glo = halves(g * cosb[k, rows, :])
                buf[i * A + r : i * A + r + 16, :M] = ghi
                buf[i * A + r : i * A + r + 16, M:] = glo

    def contract(buf, step):
        hmat = dot(buf[...], t["qb"][...])
        for i in range(KK):
            h = hmat[i * A : i * A + A]
            at = pl.ds(step * KK + i + 8, 1)
            ug[at, :] = jnp.sum(h * t["ca"][...], axis=0, keepdims=True)
            vg[at, :] = jnp.sum(h * t["sa"][...], axis=0, keepdims=True)

    def first_back(two, _):
        fill(gh, 2 * two)
        contract(gl, 2 * two - 1)
        fill(gl, 2 * two + 1)
        contract(gh, 2 * two)
        return 0

    def second_back(step, _):
        sums = [[jnp.zeros((8, 128), F32) for _ in range(NARROW)] for _ in range(KK)]
        for r in range(0, A, 16):
            rows = slice(r, r + 16)
            d = [dmix[c, rows, :] for c in range(NARROW)]
            for i in range(KK):
                b = basis[step * KK + i, rows, :]
                for c in range(NARROW):
                    e = b * d[c]
                    sums[i][c] = sums[i][c] + ((e[:8, :128] + e[:8, 128:]) + (e[8:, :128] + e[8:, 128:]))
        for i in range(KK):
            for c in range(NARROW):
                sgs[pl.ds(c * 128 + step * KK + i, 1), :] = jnp.sum(sums[i][c], axis=0, keepdims=True)
        return 0

    filter_grad(0)
    lax.fori_loop(0, ORDER // KK, half_back, 0)
    filter_grad(1)
    lax.fori_loop(0, ORDER // KK // 2, first_back, 0)
    contract(gl, ORDER // KK - 1)

    across = (((1,), (1,)), ((), ()))
    hdot = lambda a, b: lax.dot_general(a, b, across, precision=high, preferred_element_type=F32)
    lanes = lax.broadcasted_iota(jnp.int32, (1, 128), 1)
    two = lambda x: jnp.where(lanes < 2 * TERMS, x, 0.0)
    first = hdot(two(t["ea"][...]), ug[8:, :]) + hdot(two(t["eb"][...]), vg[8:, :])
    first = jnp.concatenate(
        [
            jnp.concatenate([first[:16], first[16:32]], axis=1),
            jnp.concatenate([first[32:40], jnp.zeros((8, 64), F32)], axis=1),
        ],
        axis=0,
    )

    def issue(buf, slot, value, me, count, target):
        buf[pl.ds(me, 1)] = value[None]
        for i in range(1, count):
            pltpu.make_async_remote_copy(
                src_ref=buf.at[me],
                dst_ref=buf.at[me],
                send_sem=send_sem.at[slot],
                recv_sem=recv_sem.at[slot],
                device_id=target(lax.rem(me + i, count)),
                device_id_type=MESH,
            ).start()

    def collect(buf, slot, count):
        landed(buf.at[pl.ds(0, count - 1)], recv_sem, slot)
        value = buf[0]
        for i in range(1, count):
            value = value + buf[i]
        return value

    if comm:
        issue(red_a, 7, first, ci, PEERS, lambda p: {"chan": p})

    lax.fori_loop(0, ORDER // KK, second_back, 0)
    ones = jnp.ones((8, 128), F32)
    block = jnp.concatenate([hdot(ones, sgs[c * 128 : c * 128 + 128, :])[:1] for c in range(NARROW)], axis=0)

    if not comm:
        gath[...] = jnp.zeros_like(gath)
        gath[0] = block
        first_out[...] = first
        return

    def tell(i, _):
        pltpu.make_async_remote_copy(
            src_ref=gath.at[bi],
            dst_ref=gath.at[bi],
            send_sem=send_sem.at[6],
            recv_sem=recv_sem.at[6],
            device_id={"batch": peer(i)},
            device_id_type=MESH,
        ).start()
        return 0

    zi, xy = bi // 8, lax.rem(bi, 8)
    first = collect(red_a, 7, PEERS)
    issue(red_c, 8, first, xy, 8, lambda p: {"batch": zi * 8 + p})
    gath[pl.ds(bi, 1)] = block[None]
    lax.fori_loop(0, GROUPS - 1, tell, 0)
    first = collect(red_c, 8, 8)
    issue(red_b, 9, first, zi, 8, lambda p: {"batch": p * 8 + xy})
    first_out[...] = collect(red_b, 9, 8)

    whole = y_recv.at[pl.ds(0, (GROUPS - 1) * 16)]
    landed(whole, recv_sem, 4)
    landed(gath.at[pl.ds(0, GROUPS - 1)], recv_sem, 6)
    for slot in (0, 4):
        landed(whole, send_sem, slot)
    for slot in (2, 3):
        arrived(y_recv, send_sem, slot)
    landed(gath.at[pl.ds(0, GROUPS - 1)], send_sem, 6)
    landed(red_a.at[pl.ds(0, PEERS - 1)], send_sem, 7)
    landed(red_c.at[pl.ds(0, 7)], send_sem, 8)
    landed(red_b.at[pl.ds(0, 7)], send_sem, 9)


def finish(y, gath, first, grad, first_grad, second_grad, decay_grad, skip_grad):
    for q in range(4):
        grad[:, q * 128 : q * 128 + 128] = y[pl.ds(q, 256, stride=4), :]
    turned = gath[...].T
    second_grad[...] = turned[:ORDER]
    decay_grad[...] = turned[ORDER : ORDER + 1]
    skip_grad[...] = turned[ORDER + 1 : ORDER + 2]
    first_grad[:16] = first[:16, :ORDER]
    first_grad[16:32] = first[:16, ORDER:]
    first_grad[32:33] = first[16:17, :ORDER]


def call(comm, sig, cot, first_layer, second_layer, rate, gain):
    vmem = pl.BlockSpec(memory_space=pltpu.VMEM)
    anywhere = pl.BlockSpec(memory_space=pl.ANY)
    t = tables()
    line = lambda: pltpu.VMEM((GROUPS * 16, 128), F32)
    half = lambda: pltpu.VMEM((GROUPS * 8, 128), F32)
    scratch = [pltpu.VMEM(t[name].shape, t[name].dtype) for name in NAMES]
    scratch += [
        pltpu.VMEM(sig.shape, F32),
        pltpu.VMEM(cot.shape, F32),
        pltpu.VMEM(first_layer.shape, F32),
        pltpu.SMEM(second_layer.shape, F32),
        pltpu.SMEM(rate.shape, F32),
        pltpu.SMEM(gain.shape, F32),
        line(),
        line(),
    ]
    scratch += [half(), half(), line(), line()]
    scratch += [
        pltpu.VMEM((ORDER, A, M), F32),
        pltpu.VMEM((ORDER, A, M), F32),
        pltpu.VMEM((ORDER, A, M), F32),
        pltpu.VMEM((KK * A, 128), BF16),
        pltpu.VMEM((KK * A, M), F32),
        pltpu.VMEM((NARROW, A, M), F32),
        pltpu.VMEM((NARROW, A, M), F32),
        pltpu.VMEM((A, M), BF16),
        pltpu.VMEM((A, M), BF16),
        pltpu.VMEM((NARROW * A, 2 * M), BF16),
        pltpu.VMEM((NARROW * A, 2 * M), BF16),
        pltpu.VMEM((NARROW * A, 2 * M), F32),
        pltpu.VMEM((NARROW * A, 2 * M), F32),
        pltpu.VMEM((2 * A, 2 * M), F32),
        pltpu.VMEM((2 * A, 2 * M), F32),
        pltpu.VMEM((2 * A, M), F32),
        pltpu.VMEM((NARROW * 128, 128), F32),
        pltpu.VMEM((ORDER, 128), F32),
        pltpu.VMEM((ORDER, 128), F32),
        pltpu.VMEM((ORDER + 8, 128), F32),
        pltpu.VMEM((ORDER + 8, 128), F32),
        pltpu.VMEM((PEERS, 24, 128), F32),
        pltpu.VMEM((8, 24, 128), F32),
        pltpu.VMEM((8, 24, 128), F32),
        pltpu.SemaphoreType.DMA((10,)),
        pltpu.SemaphoreType.DMA((10,)),
        pltpu.SemaphoreType.DMA((6 + len(NAMES),)),
    ]
    params = dict(vmem_limit_bytes=VMEM_LIMIT)
    if comm:
        params.update(collective_id=0, has_side_effects=True)
    return pl.pallas_call(
        functools.partial(kernel, comm),
        out_shape=(
            jax.ShapeDtypeStruct((GROUPS * 16, 128), F32),
            jax.ShapeDtypeStruct((GROUPS, NARROW, 128), F32),
            jax.ShapeDtypeStruct((24, 128), F32),
        ),
        in_specs=[anywhere] * (6 + len(NAMES)),
        out_specs=(vmem, vmem, vmem),
        scratch_shapes=scratch,
        compiler_params=pltpu.CompilerParams(**params),
        name="hyena_back",
    )(sig, cot, first_layer, second_layer, rate, gain, *[jnp.asarray(t[name]) for name in NAMES])


def local(signal, cotangent, first_layer, second_layer, decay_rate, skip_gain):
    y, gath, first = call(True, signal, cotangent, first_layer, second_layer, decay_rate, skip_gain)
    vmem = pl.BlockSpec(memory_space=pltpu.VMEM)
    grad, first_grad, second_grad, decay_grad, skip_grad = pl.pallas_call(
        finish,
        out_shape=(
            jax.ShapeDtypeStruct(signal.shape, F32),
            jax.ShapeDtypeStruct(first_layer.shape, F32),
            jax.ShapeDtypeStruct(second_layer.shape, F32),
            jax.ShapeDtypeStruct((1, decay_rate.shape[0]), F32),
            jax.ShapeDtypeStruct((1, skip_gain.shape[0]), F32),
        ),
        in_specs=[vmem] * 3,
        out_specs=(vmem,) * 5,
        name="finish",
    )(y, gath.reshape(GROUPS * NARROW, 128), first)
    return grad, first_grad, second_grad, decay_grad.reshape(-1), skip_grad.reshape(-1)


def solution(mesh):
    placed = (P("chan", "batch"), P("chan", "batch"), P(), P(None, "chan"), P("chan"), P("chan"))
    return jax.shard_map(
        local,
        mesh=mesh,
        in_specs=placed,
        out_specs=(P("chan", "batch"), P(), P(None, "chan"), P("chan"), P("chan")),
        check_vma=False,
    )
```

```python
import functools
import math

import jax
import jax.numpy as jnp
import numpy as np
from jax import lax
from jax.experimental import pallas as pl
from jax.experimental.pallas import tpu as pltpu
from jax.sharding import PartitionSpec as P

GROUPS = 64
PEERS = 4
NARROW = 4
LENGTH = 32768
LOCAL = LENGTH // GROUPS
ORDER = 64
BANDS = 16
EMBED = 33
A = 128
M = 256
TERMS = 2 * BANDS + 2
FACTOR = 1.0 / math.sqrt(LENGTH)
EPSILON = 1e-06
F32 = jnp.float32
BF16 = jnp.bfloat16
MESH = pl.DeviceIdType.MESH
SIN = (6.283185158626588, -10.33541366421067, 5.100061181598971, -1.19608076409451, 0.154421099195309)
COS = (0.9999999530044438, -4.934792784653484, 4.058410137182749, -1.331866894431586, 0.21966648431395203)
KK = 4
EARLY = 3
VMEM_LIMIT = 66300000
OUT = pltpu.VMEM
PIN = False


def split_np(x):
    hi = np.asarray(x, np.float32).astype(jnp.bfloat16)
    lo = (np.asarray(x, np.float64) - hi.astype(np.float64)).astype(jnp.bfloat16)
    return hi, lo


@functools.cache
def tables():
    row = np.arange(A)
    place = 2 * (row % 64) + row // 64
    k1 = np.arange(A)[:, None] + 0.25
    m = np.arange(M)
    phase = 2 * np.pi * k1 * place[None, :] / A
    first = np.concatenate([np.cos(phase), -np.sin(phase)], axis=0)
    twist = -2 * np.pi * k1 * m[None, :] / LENGTH
    grid = 2 * np.pi * (np.outer(m, m) % M) / M
    c, s = np.cos(grid), np.sin(grid)
    second = np.block([[c, -s], [s, c]])
    last = np.concatenate([np.cos(phase), -np.sin(phase)], axis=0).T / LENGTH
    out = {}
    out["t1h"], out["t1l"] = split_np(first)
    out["dh"], out["dl"] = split_np(second)
    out["t2h"], out["t2l"] = split_np(last)
    out["twr"] = np.cos(twist).astype(np.float32)
    out["twi"] = np.sin(twist).astype(np.float32)
    b = np.arange(1, BANDS + 1)
    alpha = 2 * np.pi * np.outer(place, b) / A
    beta = 2 * np.pi * np.outer(b, m) / LENGTH
    ones = np.ones((A, 1))
    ca = np.concatenate([np.cos(alpha), np.cos(alpha), place[:, None] / A, ones], axis=1)
    sa = np.concatenate([np.sin(alpha), np.sin(alpha), 0 * ones, 0 * ones], axis=1)
    q = np.concatenate([np.cos(beta), np.sin(beta), np.ones((1, M)), m[None, :] / LENGTH], axis=0)
    wide = lambda x: np.pad(np.tile(x, (1, 3)), ((0, 0), (0, 128 - 3 * TERMS))).astype(np.float32)
    out["ca"], out["sa"] = wide(ca), wide(sa)
    qh, rest = split_np(q)[0], None
    qm = (q - qh.astype(np.float64)).astype(jnp.bfloat16)
    out["q3"] = np.pad(np.concatenate([qh, qm, qh], axis=0), ((0, 128 - 3 * TERMS), (0, 0)))
    qb = np.zeros((2 * M, 128), jnp.bfloat16)
    qb[:M, :TERMS] = qh.T
    qb[:M, TERMS : 2 * TERMS] = qm.T
    qb[M:, :TERMS] = qh.T
    out["qb"] = qb
    e1 = np.zeros((TERMS, 40), np.float32)
    e2 = np.zeros((TERMS, 40), np.float32)
    for i in range(BANDS):
        e1[i, 1 + i] = 1
        e1[BANDS + i, 1 + BANDS + i] = 1
        e2[i, 1 + BANDS + i] = 1
        e2[BANDS + i, 1 + i] = -1
    e1[2 * BANDS :, 0] = 1
    out["ea"], out["eb"] = wide(e1.T), wide(e2.T)
    return out


NAMES = ("t1h", "t1l", "dh", "dl", "t2h", "t2l", "twr", "twi", "ca", "sa", "q3", "qb", "ea", "eb")


def halves(x):
    hi = x.astype(BF16)
    return hi, (x - hi.astype(F32)).astype(BF16)


def dot(a, b):
    return jnp.dot(a, b, preferred_element_type=F32)


def mm3(ah, al, bh, bl):
    return dot(ah, bh) + dot(al, bh) + dot(ah, bl)


def sin_cos(x):
    magic = 12582912.0
    f = x - ((x + magic) - magic)
    z = f * f
    s = SIN[4]
    for a in SIN[3::-1]:
        s = s * z + a
    s = s * f
    c = COS[4]
    for a in COS[3::-1]:
        c = c * z + a
    return s * c, 1.0 - (0.5 * s) * s


def kernel(comm, *refs):
    it = iter(refs)
    take = lambda n: [next(it) for _ in range(n)]
    sig_in, cot_in, first_in, second_in, rate_in, gain_in = take(6)
    t_in = dict(zip(NAMES, take(len(NAMES))))
    if comm:
        grad, first_grad, second_grad, decay_grad, skip_grad = take(5)
    else:
        y_recv, gath, first_out = take(3)
    t = dict(zip(NAMES, take(len(NAMES))))
    sig, cot, weights, cols, rate, gain = take(6)
    s_send, c_send = take(2)
    s_recv, c_recv, y_send = take(2), next(it), next(it)
    basis, cosb, part, pbuf, bbuf, raw, dmix = take(7)
    xh, xl, gh, gl, spec_f, spec_c, spec_s, wbuf = take(8)
    mid, sgs, u_ref, v_ref, ug, vg, red_a, red_b, red_c = take(9)
    send_sem, recv_sem, load_sem = take(3)
    if comm:
        y_recv, gath_z, gath = take(3)

    bi = lax.axis_index("batch") if comm else 0
    ci = lax.axis_index("chan") if comm else 0

    def others(visit):
        def step(i, _):
            visit(lax.rem(bi + i, GROUPS))
            return 0

        lax.fori_loop(GROUPS // 2, GROUPS, step, 0)
        lax.fori_loop(1, GROUPS // 2, step, 0)

    loads = [(cot_in, cot), (sig_in, sig), (first_in, weights), (second_in, cols), (rate_in, rate), (gain_in, gain)]
    loads += [(t_in[name], t[name]) for name in NAMES]
    loads = [pltpu.make_async_copy(src, dst, load_sem.at[i]) for i, (src, dst) in enumerate(loads)]
    for load in loads[:2]:
        load.start()

    if comm:
        barrier = pltpu.get_barrier_semaphore()

        others(lambda p: pl.semaphore_signal(barrier, inc=1, device_id={"batch": p}, device_id_type=MESH))
        for i in range(1, PEERS):
            pl.semaphore_signal(barrier, inc=1, device_id={"chan": lax.rem(ci + i, PEERS)}, device_id_type=MESH)

    for load in loads[2:]:
        load.start()

    def spread(src, dst, slot, skip, step, at, to, rows=8):
        def push(p):
            pltpu.make_async_remote_copy(
                src_ref=src.at[pl.ds(pl.multiple_of(p * skip + at, 8), rows)],
                dst_ref=dst.at[pl.ds(pl.multiple_of(bi * step + to, 8), rows)],
                send_sem=send_sem.at[slot],
                recv_sem=recv_sem.at[slot],
                device_id={"batch": p},
                device_id_type=MESH,
            ).start()

        others(push)
        own = pl.ds(pl.multiple_of(bi * step + to, 8), rows)
        dst[own, :] = src[pl.ds(pl.multiple_of(bi * skip + at, 8), rows), :]

    def landed(span, sem, slot):
        pltpu.make_async_copy(span, span, sem.at[slot]).wait()

    def arrived(buf, sem, slot):
        landed(buf.at[pl.ds(0, (GROUPS - 1) * 8)], sem, slot)

    for q in range(4 if comm else 0):
        if q == 0:
            loads[0].wait()
        c_send[pl.ds(q, 256, stride=4), :] = cot[:, q * 128 : q * 128 + 128]
    for q in range(4 if comm else 0):
        if q == 0:
            loads[1].wait()
        s_send[pl.ds(q, 256, stride=4), :] = sig[:, q * 128 : q * 128 + 128]
    if not comm:
        loads[0].wait()
        loads[1].wait()
        for h in range(2):
            for r in range(4):
                rows = pl.ds(h * 512 + r * 128, 128)
                c_recv[h * 512 + r * 128 : h * 512 + r * 128 + 128, :] = cot[rows, :]
                s_recv[h][r * 128 : r * 128 + 128, :] = sig[rows, :]
    for load in loads[2:]:
        load.wait()

    high = lax.Precision.HIGHEST
    place = bi * NARROW
    turn = (((0,), (0,)), ((), ()))
    turns = 0.5 / math.pi
    u_ref[...] = turns * lax.dot_general(weights[...], t["ea"][:EMBED], turn, precision=high, preferred_element_type=F32)
    v_ref[...] = turns * lax.dot_general(weights[...], t["eb"][:EMBED], turn, precision=high, preferred_element_type=F32)

    lane = lax.broadcasted_iota(jnp.int32, (1, 128), 1)
    raw[...] = jnp.zeros_like(raw)

    def hidden(step, _):
        for i in range(KK):
            k = step * KK + i
            for r in range(0, A, 32):
                rows = slice(r, r + 32)
                p = u_ref[pl.ds(k, 1), :] * t["ca"][rows, :] + v_ref[pl.ds(k, 1), :] * t["sa"][rows, :]
                p = jnp.where(lane < 2 * TERMS, p, p - p.astype(BF16).astype(F32))
                pbuf[i * A + r : i * A + r + 32, :] = p.astype(BF16)
        bbuf[...] = dot(pbuf[...], t["q3"][...])

        for r in range(0, A, 16):
            rows = slice(r, r + 16)
            acc = [raw[c, rows, :] for c in range(NARROW)]
            for i in range(KK):
                k = step * KK + i
                sine, cosine = sin_cos(bbuf[i * A + r : i * A + r + 16, :])
                basis[k, rows, :] = sine
                cosb[k, rows, :] = cosine
                for c in range(NARROW):
                    acc[c] = acc[c] + sine * cols[k, place + c]
            for c in range(NARROW):
                raw[c, rows, :] = acc[c]
        return 0

    lax.fori_loop(0, EARLY, hidden, 0)
    if comm:
        pl.semaphore_wait(barrier, GROUPS - 1 + PEERS - 1)
        spread(c_send, c_recv, 0, 16, 16, 0, 0, 16)
        for h in range(2):
            spread(s_send, s_recv[h], 2 + h, 16, 8, 8 * h, 0)
    lax.fori_loop(EARLY, ORDER // KK, hidden, 0)

    row = lax.broadcasted_iota(jnp.int32, (A, M), 0)
    col = lax.broadcasted_iota(jnp.int32, (A, M), 1)
    where = 512 * lax.rem(row, 64) + 256 * (row // 64) + col
    fraction = where.astype(F32) * (1.0 / LENGTH)

    def total(x):
        return jnp.sum(jnp.sum(x, axis=1, keepdims=True), axis=0, keepdims=True)

    def forward(load, spec, at, count):
        for c in range(count):
            xh[...], xl[...] = halves(load(c))
            f = mm3(t["t1h"][...], t["t1l"][...], xh[...], xl[...])
            re, im = f[:A], f[A:]
            rows = slice(c * A, c * A + A)
            gh[rows, :M], gl[rows, :M] = halves(re * t["twr"][...] - im * t["twi"][...])
            gh[rows, M:], gl[rows, M:] = halves(re * t["twi"][...] + im * t["twr"][...])
        rows = slice(0, count * A)
        spec[at * A : (at + count) * A, :] = mm3(gh[rows, :], gl[rows, :], t["dh"][...], t["dl"][...])

    def inverse(one, at, pair, store):
        for c in range(2):
            rows = slice(c * A, c * A + A)
            from_one = slice((at + c) * A, (at + c + 1) * A)
            from_two = slice((2 * pair + c) * A, (2 * pair + c + 1) * A)
            r1, i1 = one[from_one, :M], one[from_one, M:]
            r2, i2 = spec_c[from_two, :M], spec_c[from_two, M:]
            gh[rows, :M], gl[rows, :M] = halves(r1 * r2 + i1 * i2)
            gh[rows, M:], gl[rows, M:] = halves(r1 * i2 - i1 * r2)
        rows = slice(0, 2 * A)
        across = (((1,), (1,)), ((), ()))
        tdot = lambda a, b: lax.dot_general(a, b, across, preferred_element_type=F32)
        high_part, low_part = gh[rows, :], gl[rows, :]
        wbuf[...] = (
            tdot(high_part, t["dh"][...]) + tdot(low_part, t["dh"][...]) + tdot(high_part, t["dl"][...])
        )
        for c in range(2):
            rows = slice(c * A, c * A + A)
            re, im = wbuf[rows, :M], wbuf[rows, M:]
            mid[:A, :] = re * t["twr"][...] + im * t["twi"][...]
            mid[A:, :] = im * t["twr"][...] - re * t["twi"][...]
            h, low = halves(mid[...])
            store(c, mm3(t["t2h"][...], t["t2l"][...], h, low))

    def blocks_of(buf, c, stride):
        parts = [[buf[pl.ds(4 * c + 2 * h + q, 64, stride=stride), :] for q in range(2)] for h in range(2)]
        return jnp.concatenate([jnp.concatenate(p, axis=1) for p in parts], axis=0)

    norms = []
    for c in range(NARROW):
        value = raw[c] * jnp.exp(-rate[place + c] * fraction)
        raw[c] = value
        norms.append(jnp.sqrt(total(value * value) + EPSILON))
    forward(lambda c: raw[c] / norms[c], spec_f, 0, NARROW)
    sgs[...] = jnp.zeros_like(sgs)

    def store_grad(c, y):
        y = y + gain[place + c] * blocks_of(c_recv, c, 16)
        for h in range(2):
            for q in range(2):
                y_send[pl.ds(4 * c + 2 * h + q, 64, stride=16), :] = y[h * 64 : h * 64 + 64, q * 128 : q * 128 + 128]

    if comm:
        landed(c_recv.at[pl.ds(0, (GROUPS - 1) * 16)], recv_sem, 0)
    forward(lambda c: blocks_of(c_recv, c, 16), spec_c, 0, NARROW)
    for pair in range(2):
        inverse(spec_f, 2 * pair, pair, lambda c, y: store_grad(2 * pair + c, y))
    if comm:
        spread(y_send, y_recv, 4, 16, 16, 0, 0, 16)
    else:
        for r in range(8):
            y_recv[r * 128 : r * 128 + 128, :] = y_send[r * 128 : r * 128 + 128, :]

    def filter_grad(pair):
        if comm:
            arrived(s_recv[pair], recv_sem, 2 + pair)
        forward(lambda c: blocks_of(s_recv[pair], c, 8), spec_s, 0, 2)

        def store(c, y):
            ch = 2 * pair + c
            dfilt = FACTOR * y
            norm = norms[ch]
            value = raw[ch]
            filt = value / norm
            project = total(filt * dfilt)
            draw = (dfilt - filt * project) / norm
            decay = -jnp.sum(draw * value * fraction, axis=0, keepdims=True)
            skip = blocks_of(c_recv, ch, 16) * blocks_of(s_recv[pair], c, 8)
            skip = FACTOR * jnp.sum(skip, axis=0, keepdims=True)
            sgs[ch * 128 + 64 : ch * 128 + 65, :] = decay[:, :128] + decay[:, 128:]
            sgs[ch * 128 + 65 : ch * 128 + 66, :] = skip[:, :128] + skip[:, 128:]
            dmix[ch] = draw * jnp.exp(-rate[place + ch] * fraction)

        inverse(spec_s, 0, pair, store)

    def half_back(step, _):
        for r in range(0, A, 16):
            rows = slice(r, r + 16)
            d = [dmix[c, rows, :] for c in range(2)]
            for i in range(KK):
                k = step * KK + i
                part[k, rows, :] = d[0] * cols[k, place] + d[1] * cols[k, place + 1]
        return 0

    def fill(buf, step):
        for r in range(0, A, 16):
            rows = slice(r, r + 16)
            d = [dmix[c, rows, :] for c in range(2, 4)]
            for i in range(KK):
                k = step * KK + i
                g = part[k, rows, :] + d[0] * cols[k, place + 2] + d[1] * cols[k, place + 3]
                ghi, glo = halves(g * cosb[k, rows, :])
                buf[i * A + r : i * A + r + 16, :M] = ghi
                buf[i * A + r : i * A + r + 16, M:] = glo

    def contract(buf, step):
        hmat = dot(buf[...], t["qb"][...])
        for i in range(KK):
            h = hmat[i * A : i * A + A]
            at = pl.ds(step * KK + i + 8, 1)
            ug[at, :] = jnp.sum(h * t["ca"][...], axis=0, keepdims=True)
            vg[at, :] = jnp.sum(h * t["sa"][...], axis=0, keepdims=True)

    def first_back(two, _):
        fill(gh, 2 * two)
        contract(gl, 2 * two - 1)
        fill(gl, 2 * two + 1)
        contract(gh, 2 * two)
        return 0

    def second_back(pair, step, _):
        sums = [[jnp.zeros((8, 128), F32) for _ in range(2)] for _ in range(KK)]
        for r in range(0, A, 16):
            rows = slice(r, r + 16)
            d = [dmix[2 * pair + c, rows, :] for c in range(2)]
            for i in range(KK):
                b = basis[step * KK + i, rows, :]
                for c in range(2):
                    e = b * d[c]
                    sums[i][c] = sums[i][c] + ((e[:8, :128] + e[:8, 128:]) + (e[8:, :128] + e[8:, 128:]))
        for i in range(KK):
            for c in range(2):
                at = (2 * pair + c) * 128 + step * KK + i
                sgs[pl.ds(at, 1), :] = jnp.sum(sums[i][c], axis=0, keepdims=True)
        return 0

    filter_grad(0)
    lax.fori_loop(0, ORDER // KK, half_back, 0)
    lax.fori_loop(0, ORDER // KK, functools.partial(second_back, 0), 0)
    filter_grad(1)
    lax.fori_loop(0, ORDER // KK // 2, first_back, 0)
    contract(gl, ORDER // KK - 1)

    across = (((1,), (1,)), ((), ()))
    hdot = lambda a, b: lax.dot_general(a, b, across, precision=high, preferred_element_type=F32)
    lanes = lax.broadcasted_iota(jnp.int32, (1, 128), 1)
    two = lambda x: jnp.where(lanes < 2 * TERMS, x, 0.0)
    first = hdot(two(t["ea"][...]), ug[8:, :]) + hdot(two(t["eb"][...]), vg[8:, :])
    first = jnp.concatenate(
        [
            jnp.concatenate([first[:16], first[16:32]], axis=1),
            jnp.concatenate([first[32:33], jnp.zeros((1, 64), F32)], axis=1),
        ],
        axis=0,
    )

    def issue(buf, slot, value, me, count, target):
        buf[pl.ds(me, 1)] = value[None]
        for i in range(1, count):
            pltpu.make_async_remote_copy(
                src_ref=buf.at[me],
                dst_ref=buf.at[me],
                send_sem=send_sem.at[slot],
                recv_sem=recv_sem.at[slot],
                device_id=target(lax.rem(me + i, count)),
                device_id_type=MESH,
            ).start()

    def collect(buf, slot, count):
        landed(buf.at[pl.ds(0, count - 1)], recv_sem, slot)
        value = buf[0]
        for i in range(1, count):
            value = value + buf[i]
        return value

    if comm:
        issue(red_a, 7, first, ci, PEERS, lambda p: {"chan": p})

    lax.fori_loop(0, ORDER // KK, functools.partial(second_back, 1), 0)
    ones = jnp.ones((8, 128), F32)
    block = jnp.concatenate([hdot(ones, sgs[c * 128 : c * 128 + 128, :])[:1] for c in range(NARROW)], axis=0)

    if not comm:
        gath[...] = jnp.zeros_like(gath)
        gath[0] = block
        first_out[...] = first
        return

    zi, xy = bi // 8, lax.rem(bi, 8)
    along_z = lambda p: {"batch": p * 8 + xy}
    in_plane = lambda p: {"batch": zi * 8 + p}
    issue(gath_z, 5, block, zi, 8, along_z)
    first = collect(red_a, 7, PEERS)
    issue(red_c, 8, first, xy, 8, in_plane)
    landed(gath_z.at[pl.ds(0, 7)], recv_sem, 5)
    issue(gath, 6, gath_z[...], xy, 8, in_plane)
    first = collect(red_c, 8, 8)
    issue(red_b, 9, first, zi, 8, along_z)

    whole = y_recv.at[pl.ds(0, (GROUPS - 1) * 16)]
    landed(whole, recv_sem, 4)
    for q in range(4):
        grad[:, q * 128 : q * 128 + 128] = y_recv[pl.ds(q, 256, stride=4), :]
    landed(gath.at[pl.ds(0, 7)], recv_sem, 6)
    every = jnp.concatenate([gath[:, z].reshape(8 * NARROW, 128) for z in range(8)], axis=0)
    turned = every.T
    second_grad[...] = turned[:ORDER]
    decay_grad[...] = turned[ORDER : ORDER + 1]
    skip_grad[...] = turned[ORDER + 1 : ORDER + 2]
    first = collect(red_b, 9, 8)
    first_grad[:16] = first[:16, :ORDER]
    first_grad[16:32] = first[:16, ORDER:]
    first_grad[32:33] = first[16:17, :ORDER]

    for slot in (0, 4):
        landed(whole, send_sem, slot)
    for slot in (2, 3):
        arrived(y_recv, send_sem, slot)
    landed(gath_z.at[pl.ds(0, 7)], send_sem, 5)
    landed(gath.at[pl.ds(0, 7)], send_sem, 6)
    landed(red_a.at[pl.ds(0, PEERS - 1)], send_sem, 7)
    landed(red_c.at[pl.ds(0, 7)], send_sem, 8)
    landed(red_b.at[pl.ds(0, 7)], send_sem, 9)


def finish(*refs):
    sem = refs[10]
    copies = [pltpu.make_async_copy(refs[i], refs[5 + i], sem.at[i]) for i in range(5)]
    for copy in copies:
        copy.start()
    for copy in copies:
        copy.wait()


def call(comm, sig, cot, first_layer, second_layer, rate, gain):
    vmem = pl.BlockSpec(memory_space=pltpu.VMEM)
    anywhere = pl.BlockSpec(memory_space=pltpu.HBM)
    t = tables()
    line = lambda: pltpu.VMEM((GROUPS * 16, 128), F32)
    half = lambda: pltpu.VMEM((GROUPS * 8, 128), F32)
    scratch = [pltpu.VMEM(t[name].shape, t[name].dtype) for name in NAMES]
    scratch += [
        pltpu.VMEM(sig.shape, F32),
        pltpu.VMEM(cot.shape, F32),
        pltpu.VMEM(first_layer.shape, F32),
        pltpu.SMEM(second_layer.shape, F32),
        pltpu.SMEM(rate.shape, F32),
        pltpu.SMEM(gain.shape, F32),
        line(),
        line(),
    ]
    scratch += [half(), half(), line(), line()]
    scratch += [
        pltpu.VMEM((ORDER, A, M), F32),
        pltpu.VMEM((ORDER, A, M), F32),
        pltpu.VMEM((ORDER, A, M), F32),
        pltpu.VMEM((KK * A, 128), BF16),
        pltpu.VMEM((KK * A, M), F32),
        pltpu.VMEM((NARROW, A, M), F32),
        pltpu.VMEM((NARROW, A, M), F32),
        pltpu.VMEM((A, M), BF16),
        pltpu.VMEM((A, M), BF16),
        pltpu.VMEM((NARROW * A, 2 * M), BF16),
        pltpu.VMEM((NARROW * A, 2 * M), BF16),
        pltpu.VMEM((NARROW * A, 2 * M), F32),
        pltpu.VMEM((NARROW * A, 2 * M), F32),
        pltpu.VMEM((2 * A, 2 * M), F32),
        pltpu.VMEM((2 * A, 2 * M), F32),
        pltpu.VMEM((2 * A, M), F32),
        pltpu.VMEM((NARROW * 128, 128), F32),
        pltpu.VMEM((ORDER, 128), F32),
        pltpu.VMEM((ORDER, 128), F32),
        pltpu.VMEM((ORDER + 8, 128), F32),
        pltpu.VMEM((ORDER + 8, 128), F32),
        pltpu.VMEM((PEERS, 17, 128), F32),
        pltpu.VMEM((8, 17, 128), F32),
        pltpu.VMEM((8, 17, 128), F32),
        pltpu.SemaphoreType.DMA((10,)),
        pltpu.SemaphoreType.DMA((10,)),
        pltpu.SemaphoreType.DMA((6 + len(NAMES),)),
    ]
    params = dict(vmem_limit_bytes=VMEM_LIMIT)
    shapes = out_shapes(sig, first_layer, second_layer, rate, gain)
    if comm:
        scratch += [line(), pltpu.VMEM((8, NARROW, 128), F32), pltpu.VMEM((8, 8, NARROW, 128), F32)]
        params.update(collective_id=0, has_side_effects=True)
    return pl.pallas_call(
        functools.partial(kernel, comm),
        out_shape=tuple(OUT(shape, F32) for shape in shapes) if comm else tuple(
            jax.ShapeDtypeStruct(shape, F32) for shape in ((GROUPS * 16, 128), (GROUPS, NARROW, 128), (17, 128))
        ),
        in_specs=[anywhere] * (6 + len(NAMES)),
        out_specs=(vmem,) * (5 if comm else 3),
        scratch_shapes=scratch,
        compiler_params=pltpu.CompilerParams(**params),
        name="hyena_back",
    )(sig, cot, first_layer, second_layer, rate, gain, *[jnp.asarray(t[name]) for name in NAMES])


def out_shapes(sig, first_layer, second_layer, rate, gain):
    return sig.shape, first_layer.shape, second_layer.shape, (1, rate.shape[0]), (1, gain.shape[0])


def local(signal, cotangent, first_layer, second_layer, decay_rate, skip_gain):
    held = call(True, signal, cotangent, first_layer, second_layer, decay_rate, skip_gain)
    shapes = out_shapes(signal, first_layer, second_layer, decay_rate, skip_gain)
    grad, first_grad, second_grad, decay_grad, skip_grad = pl.pallas_call(
        finish,
        out_shape=tuple(jax.ShapeDtypeStruct(shape, F32) for shape in shapes),
        in_specs=[pl.BlockSpec(memory_space=pltpu.VMEM if PIN else pl.ANY)] * 5,
        out_specs=(pl.BlockSpec(memory_space=pl.ANY),) * 5,
        scratch_shapes=[pltpu.SemaphoreType.DMA((5,))],
        compiler_params=pltpu.CompilerParams(vmem_limit_bytes=4 * 2**20),
        name="finish",
    )(*held)
    return grad, first_grad, second_grad, decay_grad.reshape(-1), skip_grad.reshape(-1)


def solution(mesh):
    placed = (P("chan", "batch"), P("chan", "batch"), P(), P(None, "chan"), P("chan"), P("chan"))
    return jax.shard_map(
        local,
        mesh=mesh,
        in_specs=placed,
        out_specs=(P("chan", "batch"), P(), P(None, "chan"), P("chan"), P("chan")),
        check_vma=False,
    )
```

```python
import functools
import math

import jax
import jax.numpy as jnp
import numpy as np
from jax import lax
from jax.experimental import pallas as pl
from jax.experimental.pallas import tpu as pltpu
from jax.sharding import PartitionSpec as P

GROUPS = 64
PEERS = 4
NARROW = 4
LENGTH = 32768
LOCAL = LENGTH // GROUPS
ORDER = 64
BANDS = 16
EMBED = 33
A = 128
M = 256
TERMS = 2 * BANDS + 2
FACTOR = 1.0 / math.sqrt(LENGTH)
EPSILON = 1e-06
F32 = jnp.float32
BF16 = jnp.bfloat16
MESH = pl.DeviceIdType.MESH
SIN = (6.283185158626588, -10.33541366421067, 5.100061181598971, -1.19608076409451, 0.154421099195309)
COS = (0.9999999530044438, -4.934792784653484, 4.058410137182749, -1.331866894431586, 0.21966648431395203)
KK = 4
EARLY = 3
VMEM_LIMIT = 66300000
OUT = pltpu.VMEM
PIN = False


def split_np(x):
    hi = np.asarray(x, np.float32).astype(jnp.bfloat16)
    lo = (np.asarray(x, np.float64) - hi.astype(np.float64)).astype(jnp.bfloat16)
    return hi, lo


@functools.cache
def tables():
    row = np.arange(A)
    place = 2 * (row % 64) + row // 64
    k1 = np.arange(A)[:, None] + 0.25
    m = np.arange(M)
    phase = 2 * np.pi * k1 * place[None, :] / A
    first = np.concatenate([np.cos(phase), -np.sin(phase)], axis=0)
    twist = -2 * np.pi * k1 * m[None, :] / LENGTH
    grid = 2 * np.pi * (np.outer(m, m) % M) / M
    c, s = np.cos(grid), np.sin(grid)
    second = np.block([[c, -s], [s, c]])
    last = np.concatenate([np.cos(phase), -np.sin(phase)], axis=0).T / LENGTH
    out = {}
    out["t1h"], out["t1l"] = split_np(first)
    out["dh"], out["dl"] = split_np(second)
    out["t2h"], out["t2l"] = split_np(last)
    out["twr"] = np.cos(twist).astype(np.float32)
    out["twi"] = np.sin(twist).astype(np.float32)
    b = np.arange(1, BANDS + 1)
    alpha = 2 * np.pi * np.outer(place, b) / A
    beta = 2 * np.pi * np.outer(b, m) / LENGTH
    ones = np.ones((A, 1))
    ca = np.concatenate([np.cos(alpha), np.cos(alpha), place[:, None] / A, ones], axis=1)
    sa = np.concatenate([np.sin(alpha), np.sin(alpha), 0 * ones, 0 * ones], axis=1)
    q = np.concatenate([np.cos(beta), np.sin(beta), np.ones((1, M)), m[None, :] / LENGTH], axis=0)
    wide = lambda x: np.pad(np.tile(x, (1, 3)), ((0, 0), (0, 128 - 3 * TERMS))).astype(np.float32)
    out["ca"], out["sa"] = wide(ca), wide(sa)
    qh, rest = split_np(q)[0], None
    qm = (q - qh.astype(np.float64)).astype(jnp.bfloat16)
    out["q3"] = np.pad(np.concatenate([qh, qm, qh], axis=0), ((0, 128 - 3 * TERMS), (0, 0)))
    qb = np.zeros((2 * M, 128), jnp.bfloat16)
    qb[:M, :TERMS] = qh.T
    qb[:M, TERMS : 2 * TERMS] = qm.T
    qb[M:, :TERMS] = qh.T
    out["qb"] = qb
    e1 = np.zeros((TERMS, 40), np.float32)
    e2 = np.zeros((TERMS, 40), np.float32)
    for i in range(BANDS):
        e1[i, 1 + i] = 1
        e1[BANDS + i, 1 + BANDS + i] = 1
        e2[i, 1 + BANDS + i] = 1
        e2[BANDS + i, 1 + i] = -1
    e1[2 * BANDS :, 0] = 1
    out["ea"], out["eb"] = wide(e1.T), wide(e2.T)
    return out


NAMES = ("t1h", "t1l", "dh", "dl", "t2h", "t2l", "twr", "twi", "ca", "sa", "q3", "qb", "ea", "eb")


def halves(x):
    hi = x.astype(BF16)
    return hi, (x - hi.astype(F32)).astype(BF16)


def dot(a, b):
    return jnp.dot(a, b, preferred_element_type=F32)


def mm3(ah, al, bh, bl):
    return dot(ah, bh) + dot(al, bh) + dot(ah, bl)


def sin_cos(x):
    magic = 12582912.0
    f = x - ((x + magic) - magic)
    z = f * f
    s = SIN[4]
    for a in SIN[3::-1]:
        s = s * z + a
    s = s * f
    c = COS[4]
    for a in COS[3::-1]:
        c = c * z + a
    return s * c, 1.0 - (0.5 * s) * s


def kernel(comm, *refs):
    it = iter(refs)
    take = lambda n: [next(it) for _ in range(n)]
    sig_in, cot_in, first_in, second_in, rate_in, gain_in = take(6)
    t_in = dict(zip(NAMES, take(len(NAMES))))
    if comm:
        grad, first_grad, second_grad, decay_grad, skip_grad = take(5)
    else:
        y_recv, gath, first_out = take(3)
    t = dict(zip(NAMES, take(len(NAMES))))
    sig, cot, weights, cols, rate, gain = take(6)
    s_send, c_send = take(2)
    s_recv, c_recv, y_send = take(2), next(it), next(it)
    basis, cosb, part, pbuf, bbuf, raw, dmix = take(7)
    xh, xl, gh, gl, spec_f, spec_c, spec_s, wbuf = take(8)
    mid, sgs, u_ref, v_ref, ug, vg, red_a, red_b, red_c = take(9)
    send_sem, recv_sem, load_sem = take(3)
    if comm:
        y_recv, gath_z, gath = take(3)

    bi = lax.axis_index("batch") if comm else 0
    ci = lax.axis_index("chan") if comm else 0

    def others(visit):
        def step(i, _):
            visit(lax.rem(bi + i, GROUPS))
            return 0

        lax.fori_loop(GROUPS // 2, GROUPS, step, 0)
        lax.fori_loop(1, GROUPS // 2, step, 0)

    loads = [(cot_in, cot), (sig_in, sig), (first_in, weights), (second_in, cols), (rate_in, rate), (gain_in, gain)]
    loads += [(t_in[name], t[name]) for name in NAMES]
    loads = [pltpu.make_async_copy(src, dst, load_sem.at[i]) for i, (src, dst) in enumerate(loads)]
    for load in loads[:2]:
        load.start()

    if comm:
        barrier = pltpu.get_barrier_semaphore()

        others(lambda p: pl.semaphore_signal(barrier, inc=1, device_id={"batch": p}, device_id_type=MESH))
        for i in range(1, PEERS):
            pl.semaphore_signal(barrier, inc=1, device_id={"chan": lax.rem(ci + i, PEERS)}, device_id_type=MESH)
            across_y = {"batch": bi + 1 - 2 * lax.rem(bi, 2), "chan": lax.rem(ci + i, PEERS)}
            pl.semaphore_signal(barrier, inc=1, device_id=across_y, device_id_type=MESH)

    for load in loads[2:]:
        load.start()

    def spread(src, dst, slot, skip, step, at, to, rows=8):
        def push(p):
            pltpu.make_async_remote_copy(
                src_ref=src.at[pl.ds(pl.multiple_of(p * skip + at, 8), rows)],
                dst_ref=dst.at[pl.ds(pl.multiple_of(bi * step + to, 8), rows)],
                send_sem=send_sem.at[slot],
                recv_sem=recv_sem.at[slot],
                device_id={"batch": p},
                device_id_type=MESH,
            ).start()

        others(push)
        own = pl.ds(pl.multiple_of(bi * step + to, 8), rows)
        dst[own, :] = src[pl.ds(pl.multiple_of(bi * skip + at, 8), rows), :]

    def landed(span, sem, slot):
        pltpu.make_async_copy(span, span, sem.at[slot]).wait()

    def arrived(buf, sem, slot):
        landed(buf.at[pl.ds(0, (GROUPS - 1) * 8)], sem, slot)

    for q in range(4 if comm else 0):
        if q == 0:
            loads[0].wait()
        c_send[pl.ds(q, 256, stride=4), :] = cot[:, q * 128 : q * 128 + 128]
    for q in range(4 if comm else 0):
        if q == 0:
            loads[1].wait()
        s_send[pl.ds(q, 256, stride=4), :] = sig[:, q * 128 : q * 128 + 128]
    if not comm:
        loads[0].wait()
        loads[1].wait()
        for h in range(2):
            for r in range(4):
                rows = pl.ds(h * 512 + r * 128, 128)
                c_recv[h * 512 + r * 128 : h * 512 + r * 128 + 128, :] = cot[rows, :]
                s_recv[h][r * 128 : r * 128 + 128, :] = sig[rows, :]
    for load in loads[2:]:
        load.wait()

    high = lax.Precision.HIGHEST
    place = bi * NARROW
    turn = (((0,), (0,)), ((), ()))
    turns = 0.5 / math.pi
    u_ref[...] = turns * lax.dot_general(weights[...], t["ea"][:EMBED], turn, precision=high, preferred_element_type=F32)
    v_ref[...] = turns * lax.dot_general(weights[...], t["eb"][:EMBED], turn, precision=high, preferred_element_type=F32)

    lane = lax.broadcasted_iota(jnp.int32, (1, 128), 1)
    raw[...] = jnp.zeros_like(raw)

    def hidden(step, _):
        for i in range(KK):
            k = step * KK + i
            for r in range(0, A, 32):
                rows = slice(r, r + 32)
                p = u_ref[pl.ds(k, 1), :] * t["ca"][rows, :] + v_ref[pl.ds(k, 1), :] * t["sa"][rows, :]
                p = jnp.where(lane < 2 * TERMS, p, p - p.astype(BF16).astype(F32))
                pbuf[i * A + r : i * A + r + 32, :] = p.astype(BF16)
        bbuf[...] = dot(pbuf[...], t["q3"][...])

        for r in range(0, A, 16):
            rows = slice(r, r + 16)
            acc = [raw[c, rows, :] for c in range(NARROW)]
            for i in range(KK):
                k = step * KK + i
                sine, cosine = sin_cos(bbuf[i * A + r : i * A + r + 16, :])
                basis[k, rows, :] = sine
                cosb[k, rows, :] = cosine
                for c in range(NARROW):
                    acc[c] = acc[c] + sine * cols[k, place + c]
            for c in range(NARROW):
                raw[c, rows, :] = acc[c]
        return 0

    lax.fori_loop(0, EARLY, hidden, 0)
    if comm:
        pl.semaphore_wait(barrier, GROUPS - 1 + 2 * (PEERS - 1))
        spread(c_send, c_recv, 0, 16, 16, 0, 0, 16)
        for h in range(2):
            spread(s_send, s_recv[h], 2 + h, 16, 8, 8 * h, 0)
    lax.fori_loop(EARLY, ORDER // KK, hidden, 0)

    row = lax.broadcasted_iota(jnp.int32, (A, M), 0)
    col = lax.broadcasted_iota(jnp.int32, (A, M), 1)
    where = 512 * lax.rem(row, 64) + 256 * (row // 64) + col
    fraction = where.astype(F32) * (1.0 / LENGTH)

    def total(x):
        return jnp.sum(jnp.sum(x, axis=1, keepdims=True), axis=0, keepdims=True)

    def forward(load, spec, at, count):
        for c in range(count):
            xh[...], xl[...] = halves(load(c))
            f = mm3(t["t1h"][...], t["t1l"][...], xh[...], xl[...])
            re, im = f[:A], f[A:]
            rows = slice(c * A, c * A + A)
            gh[rows, :M], gl[rows, :M] = halves(re * t["twr"][...] - im * t["twi"][...])
            gh[rows, M:], gl[rows, M:] = halves(re * t["twi"][...] + im * t["twr"][...])
        rows = slice(0, count * A)
        spec[at * A : (at + count) * A, :] = mm3(gh[rows, :], gl[rows, :], t["dh"][...], t["dl"][...])

    def inverse(one, at, pair, store):
        for c in range(2):
            rows = slice(c * A, c * A + A)
            from_one = slice((at + c) * A, (at + c + 1) * A)
            from_two = slice((2 * pair + c) * A, (2 * pair + c + 1) * A)
            r1, i1 = one[from_one, :M], one[from_one, M:]
            r2, i2 = spec_c[from_two, :M], spec_c[from_two, M:]
            gh[rows, :M], gl[rows, :M] = halves(r1 * r2 + i1 * i2)
            gh[rows, M:], gl[rows, M:] = halves(r1 * i2 - i1 * r2)
        rows = slice(0, 2 * A)
        across = (((1,), (1,)), ((), ()))
        tdot = lambda a, b: lax.dot_general(a, b, across, preferred_element_type=F32)
        high_part, low_part = gh[rows, :], gl[rows, :]
        wbuf[...] = (
            tdot(high_part, t["dh"][...]) + tdot(low_part, t["dh"][...]) + tdot(high_part, t["dl"][...])
        )
        for c in range(2):
            rows = slice(c * A, c * A + A)
            re, im = wbuf[rows, :M], wbuf[rows, M:]
            mid[:A, :] = re * t["twr"][...] + im * t["twi"][...]
            mid[A:, :] = im * t["twr"][...] - re * t["twi"][...]
            h, low = halves(mid[...])
            store(c, mm3(t["t2h"][...], t["t2l"][...], h, low))

    def blocks_of(buf, c, stride):
        parts = [[buf[pl.ds(4 * c + 2 * h + q, 64, stride=stride), :] for q in range(2)] for h in range(2)]
        return jnp.concatenate([jnp.concatenate(p, axis=1) for p in parts], axis=0)

    norms = []
    for c in range(NARROW):
        value = raw[c] * jnp.exp(-rate[place + c] * fraction)
        raw[c] = value
        norms.append(jnp.sqrt(total(value * value) + EPSILON))
    forward(lambda c: raw[c] / norms[c], spec_f, 0, NARROW)
    sgs[...] = jnp.zeros_like(sgs)

    def store_grad(c, y):
        y = y + gain[place + c] * blocks_of(c_recv, c, 16)
        for h in range(2):
            for q in range(2):
                y_send[pl.ds(4 * c + 2 * h + q, 64, stride=16), :] = y[h * 64 : h * 64 + 64, q * 128 : q * 128 + 128]

    if comm:
        landed(c_recv.at[pl.ds(0, (GROUPS - 1) * 16)], recv_sem, 0)
    forward(lambda c: blocks_of(c_recv, c, 16), spec_c, 0, NARROW)
    for pair in range(2):
        inverse(spec_f, 2 * pair, pair, lambda c, y: store_grad(2 * pair + c, y))
    if comm:
        spread(y_send, y_recv, 4, 16, 16, 0, 0, 16)
    else:
        for r in range(8):
            y_recv[r * 128 : r * 128 + 128, :] = y_send[r * 128 : r * 128 + 128, :]

    def filter_grad(pair):
        if comm:
            arrived(s_recv[pair], recv_sem, 2 + pair)
        forward(lambda c: blocks_of(s_recv[pair], c, 8), spec_s, 0, 2)

        def store(c, y):
            ch = 2 * pair + c
            dfilt = FACTOR * y
            norm = norms[ch]
            value = raw[ch]
            filt = value / norm
            project = total(filt * dfilt)
            draw = (dfilt - filt * project) / norm
            decay = -jnp.sum(draw * value * fraction, axis=0, keepdims=True)
            skip = blocks_of(c_recv, ch, 16) * blocks_of(s_recv[pair], c, 8)
            skip = FACTOR * jnp.sum(skip, axis=0, keepdims=True)
            sgs[ch * 128 + 64 : ch * 128 + 65, :] = decay[:, :128] + decay[:, 128:]
            sgs[ch * 128 + 65 : ch * 128 + 66, :] = skip[:, :128] + skip[:, 128:]
            dmix[ch] = draw * jnp.exp(-rate[place + ch] * fraction)

        inverse(spec_s, 0, pair, store)

    def half_back(step, _):
        for r in range(0, A, 16):
            rows = slice(r, r + 16)
            d = [dmix[c, rows, :] for c in range(2)]
            for i in range(KK):
                k = step * KK + i
                part[k, rows, :] = d[0] * cols[k, place] + d[1] * cols[k, place + 1]
        return 0

    def fill(buf, step):
        for r in range(0, A, 16):
            rows = slice(r, r + 16)
            d = [dmix[c, rows, :] for c in range(2, 4)]
            for i in range(KK):
                k = step * KK + i
                g = part[k, rows, :] + d[0] * cols[k, place + 2] + d[1] * cols[k, place + 3]
                ghi, glo = halves(g * cosb[k, rows, :])
                buf[i * A + r : i * A + r + 16, :M] = ghi
                buf[i * A + r : i * A + r + 16, M:] = glo

    def contract(buf, step):
        hmat = dot(buf[...], t["qb"][...])
        for i in range(KK):
            h = hmat[i * A : i * A + A]
            at = pl.ds(step * KK + i + 8, 1)
            ug[at, :] = jnp.sum(h * t["ca"][...], axis=0, keepdims=True)
            vg[at, :] = jnp.sum(h * t["sa"][...], axis=0, keepdims=True)

    def first_back(two, _):
        fill(gh, 2 * two)
        contract(gl, 2 * two - 1)
        fill(gl, 2 * two + 1)
        contract(gh, 2 * two)
        return 0

    def second_back(pair, step, _):
        sums = [[jnp.zeros((8, 128), F32) for _ in range(2)] for _ in range(KK)]
        for r in range(0, A, 16):
            rows = slice(r, r + 16)
            d = [dmix[2 * pair + c, rows, :] for c in range(2)]
            for i in range(KK):
                b = basis[step * KK + i, rows, :]
                for c in range(2):
                    e = b * d[c]
                    sums[i][c] = sums[i][c] + ((e[:8, :128] + e[:8, 128:]) + (e[8:, :128] + e[8:, 128:]))
        for i in range(KK):
            for c in range(2):
                at = (2 * pair + c) * 128 + step * KK + i
                sgs[pl.ds(at, 1), :] = jnp.sum(sums[i][c], axis=0, keepdims=True)
        return 0

    filter_grad(0)
    lax.fori_loop(0, ORDER // KK, half_back, 0)
    lax.fori_loop(0, ORDER // KK, functools.partial(second_back, 0), 0)
    filter_grad(1)
    lax.fori_loop(0, ORDER // KK // 2, first_back, 0)
    contract(gl, ORDER // KK - 1)

    across = (((1,), (1,)), ((), ()))
    hdot = lambda a, b: lax.dot_general(a, b, across, precision=high, preferred_element_type=F32)
    lanes = lax.broadcasted_iota(jnp.int32, (1, 128), 1)
    two = lambda x: jnp.where(lanes < 2 * TERMS, x, 0.0)
    picks = jnp.concatenate([two(t["ea"][...]), two(t["eb"][...])], axis=1).astype(BF16)
    rest = jnp.concatenate([ug[8:, :], vg[8:, :]], axis=1)
    first = jnp.zeros((40, ORDER), F32)
    for _ in range(3):
        piece = rest.astype(BF16)
        rest = rest - piece.astype(F32)
        first = first + lax.dot_general(picks, piece, across, preferred_element_type=F32)
    first = jnp.concatenate(
        [
            jnp.concatenate([first[:16], first[16:32]], axis=1),
            jnp.concatenate([first[32:33], jnp.zeros((1, 64), F32)], axis=1),
        ],
        axis=0,
    )

    def issue(buf, slot, value, me, count, target):
        buf[pl.ds(me, 1)] = value[None]
        for i in range(1, count):
            pltpu.make_async_remote_copy(
                src_ref=buf.at[me],
                dst_ref=buf.at[me],
                send_sem=send_sem.at[slot],
                recv_sem=recv_sem.at[slot],
                device_id=target(lax.rem(me + i, count)),
                device_id_type=MESH,
            ).start()

    def collect(buf, slot, count):
        landed(buf.at[pl.ds(0, count - 1)], recv_sem, slot)
        value = buf[0]
        for i in range(1, count):
            value = value + buf[i]
        return value

    zi, xi, yi, xy = bi // 8, lax.rem(bi // 2, 4), lax.rem(bi, 2), lax.rem(bi, 8)
    along_y = lambda p: {"batch": bi - yi + p // PEERS, "chan": lax.rem(p, PEERS)}
    along_x = lambda p: {"batch": zi * 8 + p * 2 + yi}
    along_z = lambda p: {"batch": p * 8 + xy}
    in_plane = lambda p: {"batch": zi * 8 + p}
    if comm:
        issue(red_a, 7, first, yi * PEERS + ci, 8, along_y)

    lax.fori_loop(0, ORDER // KK, functools.partial(second_back, 1), 0)
    ones = jnp.ones((8, 128), F32)
    block = jnp.concatenate([hdot(ones, sgs[c * 128 : c * 128 + 128, :])[:1] for c in range(NARROW)], axis=0)

    if not comm:
        gath[...] = jnp.zeros_like(gath)
        gath[0] = block
        first_out[...] = first
        return

    issue(gath_z, 5, block, zi, 8, along_z)
    first = collect(red_a, 7, 8)
    issue(red_c, 8, first, xi, 4, along_x)
    landed(gath_z.at[pl.ds(0, 7)], recv_sem, 5)
    issue(gath, 6, gath_z[...], xy, 8, in_plane)
    first = collect(red_c, 8, 4)
    issue(red_b, 9, first, zi, 8, along_z)

    whole = y_recv.at[pl.ds(0, (GROUPS - 1) * 16)]
    landed(whole, recv_sem, 4)
    for q in range(4):
        grad[:, q * 128 : q * 128 + 128] = y_recv[pl.ds(q, 256, stride=4), :]
    landed(gath.at[pl.ds(0, 7)], recv_sem, 6)
    every = jnp.concatenate([gath[:, z].reshape(8 * NARROW, 128) for z in range(8)], axis=0)
    turned = every.T
    second_grad[...] = turned[:ORDER]
    decay_grad[...] = turned[ORDER : ORDER + 1]
    skip_grad[...] = turned[ORDER + 1 : ORDER + 2]
    first = collect(red_b, 9, 8)
    first_grad[:16] = first[:16, :ORDER]
    first_grad[16:32] = first[:16, ORDER:]
    first_grad[32:33] = first[16:17, :ORDER]

    for slot in (0, 4):
        landed(whole, send_sem, slot)
    for slot in (2, 3):
        arrived(y_recv, send_sem, slot)
    landed(gath_z.at[pl.ds(0, 7)], send_sem, 5)
    landed(gath.at[pl.ds(0, 7)], send_sem, 6)
    landed(red_a.at[pl.ds(0, 7)], send_sem, 7)
    landed(red_c.at[pl.ds(0, 3)], send_sem, 8)
    landed(red_b.at[pl.ds(0, 7)], send_sem, 9)


def finish(*refs):
    sem = refs[10]
    copies = [pltpu.make_async_copy(refs[i], refs[5 + i], sem.at[i]) for i in range(5)]
    for copy in copies:
        copy.start()
    for copy in copies:
        copy.wait()


def call(comm, sig, cot, first_layer, second_layer, rate, gain):
    vmem = pl.BlockSpec(memory_space=pltpu.VMEM)
    anywhere = pl.BlockSpec(memory_space=pltpu.HBM)
    t = tables()
    line = lambda: pltpu.VMEM((GROUPS * 16, 128), F32)
    half = lambda: pltpu.VMEM((GROUPS * 8, 128), F32)
    scratch = [pltpu.VMEM(t[name].shape, t[name].dtype) for name in NAMES]
    scratch += [
        pltpu.VMEM(sig.shape, F32),
        pltpu.VMEM(cot.shape, F32),
        pltpu.VMEM(first_layer.shape, F32),
        pltpu.SMEM(second_layer.shape, F32),
        pltpu.SMEM(rate.shape, F32),
        pltpu.SMEM(gain.shape, F32),
        line(),
        line(),
    ]
    scratch += [half(), half(), line(), line()]
    scratch += [
        pltpu.VMEM((ORDER, A, M), F32),
        pltpu.VMEM((ORDER, A, M), F32),
        pltpu.VMEM((ORDER, A, M), F32),
        pltpu.VMEM((KK * A, 128), BF16),
        pltpu.VMEM((KK * A, M), F32),
        pltpu.VMEM((NARROW, A, M), F32),
        pltpu.VMEM((NARROW, A, M), F32),
        pltpu.VMEM((A, M), BF16),
        pltpu.VMEM((A, M), BF16),
        pltpu.VMEM((NARROW * A, 2 * M), BF16),
        pltpu.VMEM((NARROW * A, 2 * M), BF16),
        pltpu.VMEM((NARROW * A, 2 * M), F32),
        pltpu.VMEM((NARROW * A, 2 * M), F32),
        pltpu.VMEM((2 * A, 2 * M), F32),
        pltpu.VMEM((2 * A, 2 * M), F32),
        pltpu.VMEM((2 * A, M), F32),
        pltpu.VMEM((NARROW * 128, 128), F32),
        pltpu.VMEM((ORDER, 128), F32),
        pltpu.VMEM((ORDER, 128), F32),
        pltpu.VMEM((ORDER + 8, 128), F32),
        pltpu.VMEM((ORDER + 8, 128), F32),
        pltpu.VMEM((8, 17, 128), F32),
        pltpu.VMEM((8, 17, 128), F32),
        pltpu.VMEM((4, 17, 128), F32),
        pltpu.SemaphoreType.DMA((10,)),
        pltpu.SemaphoreType.DMA((10,)),
        pltpu.SemaphoreType.DMA((6 + len(NAMES),)),
    ]
    params = dict(vmem_limit_bytes=VMEM_LIMIT)
    shapes = out_shapes(sig, first_layer, second_layer, rate, gain)
    if comm:
        scratch += [line(), pltpu.VMEM((8, NARROW, 128), F32), pltpu.VMEM((8, 8, NARROW, 128), F32)]
        params.update(collective_id=0, has_side_effects=True)
    return pl.pallas_call(
        functools.partial(kernel, comm),
        out_shape=tuple(OUT(shape, F32) for shape in shapes) if comm else tuple(
            jax.ShapeDtypeStruct(shape, F32) for shape in ((GROUPS * 16, 128), (GROUPS, NARROW, 128), (17, 128))
        ),
        in_specs=[anywhere] * (6 + len(NAMES)),
        out_specs=(vmem,) * (5 if comm else 3),
        scratch_shapes=scratch,
        compiler_params=pltpu.CompilerParams(**params),
        name="hyena_back",
    )(sig, cot, first_layer, second_layer, rate, gain, *[jnp.asarray(t[name]) for name in NAMES])


def out_shapes(sig, first_layer, second_layer, rate, gain):
    return sig.shape, first_layer.shape, second_layer.shape, (1, rate.shape[0]), (1, gain.shape[0])


def local(signal, cotangent, first_layer, second_layer, decay_rate, skip_gain):
    held = call(True, signal, cotangent, first_layer, second_layer, decay_rate, skip_gain)
    shapes = out_shapes(signal, first_layer, second_layer, decay_rate, skip_gain)
    grad, first_grad, second_grad, decay_grad, skip_grad = pl.pallas_call(
        finish,
        out_shape=tuple(jax.ShapeDtypeStruct(shape, F32) for shape in shapes),
        in_specs=[pl.BlockSpec(memory_space=pltpu.VMEM if PIN else pl.ANY)] * 5,
        out_specs=(pl.BlockSpec(memory_space=pl.ANY),) * 5,
        scratch_shapes=[pltpu.SemaphoreType.DMA((5,))],
        compiler_params=pltpu.CompilerParams(vmem_limit_bytes=4 * 2**20),
        name="finish",
    )(*held)
    return grad, first_grad, second_grad, decay_grad.reshape(-1), skip_grad.reshape(-1)


def solution(mesh):
    placed = (P("chan", "batch"), P("chan", "batch"), P(), P(None, "chan"), P("chan"), P("chan"))
    return jax.shard_map(
        local,
        mesh=mesh,
        in_specs=placed,
        out_specs=(P("chan", "batch"), P(), P(None, "chan"), P("chan"), P("chan")),
        check_vma=False,
    )
```

```python
import functools
import math

import jax
import jax.numpy as jnp
import numpy as np
from jax import lax
from jax.experimental import pallas as pl
from jax.experimental.pallas import tpu as pltpu
from jax.sharding import PartitionSpec as P

GROUPS = 64
PEERS = 4
NARROW = 4
LENGTH = 32768
LOCAL = LENGTH // GROUPS
ORDER = 64
BANDS = 16
EMBED = 33
A = 128
M = 256
TERMS = 2 * BANDS + 2
FACTOR = 1.0 / math.sqrt(LENGTH)
EPSILON = 1e-06
F32 = jnp.float32
BF16 = jnp.bfloat16
MESH = pl.DeviceIdType.MESH
SIN = (6.283185158626588, -10.33541366421067, 5.100061181598971, -1.19608076409451, 0.154421099195309)
COS = (0.9999999530044438, -4.934792784653484, 4.058410137182749, -1.331866894431586, 0.21966648431395203)
KK = 4
EARLY = 3
VMEM_LIMIT = 66300000
OUT = pltpu.VMEM
PIN = False


def split_np(x):
    hi = np.asarray(x, np.float32).astype(jnp.bfloat16)
    lo = (np.asarray(x, np.float64) - hi.astype(np.float64)).astype(jnp.bfloat16)
    return hi, lo


@functools.cache
def tables():
    row = np.arange(A)
    place = 2 * (row % 64) + row // 64
    k1 = np.arange(A)[:, None] + 0.25
    m = np.arange(M)
    phase = 2 * np.pi * k1 * place[None, :] / A
    first = np.concatenate([np.cos(phase), -np.sin(phase)], axis=0)
    twist = -2 * np.pi * k1 * m[None, :] / LENGTH
    grid = 2 * np.pi * (np.outer(m, m) % M) / M
    c, s = np.cos(grid), np.sin(grid)
    second = np.block([[c, -s], [s, c]])
    last = np.concatenate([np.cos(phase), -np.sin(phase)], axis=0).T / LENGTH
    out = {}
    out["t1h"], out["t1l"] = split_np(first)
    out["dh"], out["dl"] = split_np(second)
    out["t2h"], out["t2l"] = split_np(last)
    out["twr"] = np.cos(twist).astype(np.float32)
    out["twi"] = np.sin(twist).astype(np.float32)
    b = np.arange(1, BANDS + 1)
    alpha = 2 * np.pi * np.outer(place, b) / A
    beta = 2 * np.pi * np.outer(b, m) / LENGTH
    ones = np.ones((A, 1))
    ca = np.concatenate([np.cos(alpha), np.cos(alpha), place[:, None] / A, ones], axis=1)
    sa = np.concatenate([np.sin(alpha), np.sin(alpha), 0 * ones, 0 * ones], axis=1)
    q = np.concatenate([np.cos(beta), np.sin(beta), np.ones((1, M)), m[None, :] / LENGTH], axis=0)
    wide = lambda x: np.pad(np.tile(x, (1, 3)), ((0, 0), (0, 128 - 3 * TERMS))).astype(np.float32)
    out["ca"], out["sa"] = wide(ca), wide(sa)
    qh, rest = split_np(q)[0], None
    qm = (q - qh.astype(np.float64)).astype(jnp.bfloat16)
    out["q3"] = np.pad(np.concatenate([qh, qm, qh], axis=0), ((0, 128 - 3 * TERMS), (0, 0)))
    qb = np.zeros((2 * M, 128), jnp.bfloat16)
    qb[:M, :TERMS] = qh.T
    qb[:M, TERMS : 2 * TERMS] = qm.T
    qb[M:, :TERMS] = qh.T
    out["qb"] = qb
    e1 = np.zeros((TERMS, 40), np.float32)
    e2 = np.zeros((TERMS, 40), np.float32)
    for i in range(BANDS):
        e1[i, 1 + i] = 1
        e1[BANDS + i, 1 + BANDS + i] = 1
        e2[i, 1 + BANDS + i] = 1
        e2[BANDS + i, 1 + i] = -1
    e1[2 * BANDS :, 0] = 1
    out["ea"], out["eb"] = wide(e1.T), wide(e2.T)
    return out


NAMES = ("t1h", "t1l", "dh", "dl", "t2h", "t2l", "twr", "twi", "ca", "sa", "q3", "qb", "ea", "eb")


def halves(x):
    hi = x.astype(BF16)
    return hi, (x - hi.astype(F32)).astype(BF16)


def dot(a, b):
    return jnp.dot(a, b, preferred_element_type=F32)


def mm3(ah, al, bh, bl):
    return dot(ah, bh) + dot(al, bh) + dot(ah, bl)


def sin_cos(x):
    magic = 12582912.0
    f = x - ((x + magic) - magic)
    z = f * f
    s = SIN[4]
    for a in SIN[3::-1]:
        s = s * z + a
    s = s * f
    c = COS[4]
    for a in COS[3::-1]:
        c = c * z + a
    return s * c, 1.0 - (0.5 * s) * s


def kernel(comm, *refs):
    it = iter(refs)
    take = lambda n: [next(it) for _ in range(n)]
    sig_in, cot_in, first_in, second_in, rate_in, gain_in = take(6)
    t_in = dict(zip(NAMES, take(len(NAMES))))
    if comm:
        grad, first_grad, second_grad, decay_grad, skip_grad = take(5)
    else:
        y_recv, gath, first_out = take(3)
    t = dict(zip(NAMES, take(len(NAMES))))
    sig, cot, weights, cols, rate, gain = take(6)
    s_send, c_send = take(2)
    s_recv, c_recv, y_send = take(2), next(it), next(it)
    basis, cosb, part, pbuf, bbuf, raw, dmix = take(7)
    xh, xl, gh, gl, spec_f, spec_c, spec_s, wbuf = take(8)
    mid, sgs, u_ref, v_ref, ug, vg, red_a, red_b, red_c = take(9)
    send_sem, recv_sem, load_sem = take(3)
    if comm:
        y_recv, gath_z, gath = take(3)

    bi = lax.axis_index("batch") if comm else 0
    ci = lax.axis_index("chan") if comm else 0

    def others(visit):
        def step(p, _):
            visit(p)
            return 0

        half = GROUPS // 2
        lax.fori_loop(bi + half, GROUPS, step, 0)
        lax.fori_loop(jnp.maximum(bi - half, 0), bi, step, 0)
        lax.fori_loop(bi + 1, jnp.minimum(bi + half, GROUPS), step, 0)
        lax.fori_loop(0, bi - half, step, 0)

    loads = [(cot_in, cot), (sig_in, sig), (first_in, weights), (second_in, cols), (rate_in, rate), (gain_in, gain)]
    loads += [(t_in[name], t[name]) for name in NAMES]
    loads = [pltpu.make_async_copy(src, dst, load_sem.at[i]) for i, (src, dst) in enumerate(loads)]
    for load in loads[:2]:
        load.start()

    if comm:
        barrier = pltpu.get_barrier_semaphore()

        others(lambda p: pl.semaphore_signal(barrier, inc=1, device_id={"batch": p}, device_id_type=MESH))
        for i in range(1, PEERS):
            pl.semaphore_signal(barrier, inc=1, device_id={"chan": lax.rem(ci + i, PEERS)}, device_id_type=MESH)
            across_y = {"batch": bi + 1 - 2 * lax.rem(bi, 2), "chan": lax.rem(ci + i, PEERS)}
            pl.semaphore_signal(barrier, inc=1, device_id=across_y, device_id_type=MESH)

    for load in loads[2:]:
        load.start()

    def spread(src, dst, slot, skip, step, at, to, rows=8):
        def push(p):
            pltpu.make_async_remote_copy(
                src_ref=src.at[pl.ds(pl.multiple_of(p * skip + at, 8), rows)],
                dst_ref=dst.at[pl.ds(pl.multiple_of(bi * step + to, 8), rows)],
                send_sem=send_sem.at[slot],
                recv_sem=recv_sem.at[slot],
                device_id={"batch": p},
                device_id_type=MESH,
            ).start()

        others(push)
        own = pl.ds(pl.multiple_of(bi * step + to, 8), rows)
        dst[own, :] = src[pl.ds(pl.multiple_of(bi * skip + at, 8), rows), :]

    def landed(span, sem, slot):
        pltpu.make_async_copy(span, span, sem.at[slot]).wait()

    def arrived(buf, sem, slot):
        landed(buf.at[pl.ds(0, (GROUPS - 1) * 8)], sem, slot)

    for q in range(4 if comm else 0):
        if q == 0:
            loads[0].wait()
        c_send[pl.ds(q, 256, stride=4), :] = cot[:, q * 128 : q * 128 + 128]
    for q in range(4 if comm else 0):
        if q == 0:
            loads[1].wait()
        s_send[pl.ds(q, 256, stride=4), :] = sig[:, q * 128 : q * 128 + 128]
    if not comm:
        loads[0].wait()
        loads[1].wait()
        for h in range(2):
            for r in range(4):
                rows = pl.ds(h * 512 + r * 128, 128)
                c_recv[h * 512 + r * 128 : h * 512 + r * 128 + 128, :] = cot[rows, :]
                s_recv[h][r * 128 : r * 128 + 128, :] = sig[rows, :]
    for load in loads[2:]:
        load.wait()

    high = lax.Precision.HIGHEST
    place = bi * NARROW
    turn = (((0,), (0,)), ((), ()))
    turns = 0.5 / math.pi
    u_ref[...] = turns * lax.dot_general(weights[...], t["ea"][:EMBED], turn, precision=high, preferred_element_type=F32)
    v_ref[...] = turns * lax.dot_general(weights[...], t["eb"][:EMBED], turn, precision=high, preferred_element_type=F32)

    lane = lax.broadcasted_iota(jnp.int32, (1, 128), 1)
    raw[...] = jnp.zeros_like(raw)

    def hidden(step, _):
        for i in range(KK):
            k = step * KK + i
            for r in range(0, A, 32):
                rows = slice(r, r + 32)
                p = u_ref[pl.ds(k, 1), :] * t["ca"][rows, :] + v_ref[pl.ds(k, 1), :] * t["sa"][rows, :]
                p = jnp.where(lane < 2 * TERMS, p, p - p.astype(BF16).astype(F32))
                pbuf[i * A + r : i * A + r + 32, :] = p.astype(BF16)
        bbuf[...] = dot(pbuf[...], t["q3"][...])

        for r in range(0, A, 16):
            rows = slice(r, r + 16)
            acc = [raw[c, rows, :] for c in range(NARROW)]
            for i in range(KK):
                k = step * KK + i
                sine, cosine = sin_cos(bbuf[i * A + r : i * A + r + 16, :])
                basis[k, rows, :] = sine
                cosb[k, rows, :] = cosine
                for c in range(NARROW):
                    acc[c] = acc[c] + sine * cols[k, place + c]
            for c in range(NARROW):
                raw[c, rows, :] = acc[c]
        return 0

    lax.fori_loop(0, EARLY, hidden, 0)
    if comm:
        pl.semaphore_wait(barrier, GROUPS - 1 + 2 * (PEERS - 1))
        spread(c_send, c_recv, 0, 16, 16, 0, 0, 16)
        for h in range(2):
            spread(s_send, s_recv[h], 2 + h, 16, 8, 8 * h, 0)
    lax.fori_loop(EARLY, ORDER // KK, hidden, 0)

    row = lax.broadcasted_iota(jnp.int32, (A, M), 0)
    col = lax.broadcasted_iota(jnp.int32, (A, M), 1)
    where = 512 * lax.rem(row, 64) + 256 * (row // 64) + col
    fraction = where.astype(F32) * (1.0 / LENGTH)

    def total(x):
        return jnp.sum(jnp.sum(x, axis=1, keepdims=True), axis=0, keepdims=True)

    def forward(load, spec, at, count):
        for c in range(count):
            xh[...], xl[...] = halves(load(c))
            f = mm3(t["t1h"][...], t["t1l"][...], xh[...], xl[...])
            re, im = f[:A], f[A:]
            rows = slice(c * A, c * A + A)
            gh[rows, :M], gl[rows, :M] = halves(re * t["twr"][...] - im * t["twi"][...])
            gh[rows, M:], gl[rows, M:] = halves(re * t["twi"][...] + im * t["twr"][...])
        rows = slice(0, count * A)
        spec[at * A : (at + count) * A, :] = mm3(gh[rows, :], gl[rows, :], t["dh"][...], t["dl"][...])

    def inverse(one, at, pair, store):
        for c in range(2):
            rows = slice(c * A, c * A + A)
            from_one = slice((at + c) * A, (at + c + 1) * A)
            from_two = slice((2 * pair + c) * A, (2 * pair + c + 1) * A)
            r1, i1 = one[from_one, :M], one[from_one, M:]
            r2, i2 = spec_c[from_two, :M], spec_c[from_two, M:]
            gh[rows, :M], gl[rows, :M] = halves(r1 * r2 + i1 * i2)
            gh[rows, M:], gl[rows, M:] = halves(r1 * i2 - i1 * r2)
        rows = slice(0, 2 * A)
        across = (((1,), (1,)), ((), ()))
        tdot = lambda a, b: lax.dot_general(a, b, across, preferred_element_type=F32)
        high_part, low_part = gh[rows, :], gl[rows, :]
        wbuf[...] = (
            tdot(high_part, t["dh"][...]) + tdot(low_part, t["dh"][...]) + tdot(high_part, t["dl"][...])
        )
        for c in range(2):
            rows = slice(c * A, c * A + A)
            re, im = wbuf[rows, :M], wbuf[rows, M:]
            mid[:A, :] = re * t["twr"][...] + im * t["twi"][...]
            mid[A:, :] = im * t["twr"][...] - re * t["twi"][...]
            h, low = halves(mid[...])
            store(c, mm3(t["t2h"][...], t["t2l"][...], h, low))

    def blocks_of(buf, c, stride):
        parts = [[buf[pl.ds(4 * c + 2 * h + q, 64, stride=stride), :] for q in range(2)] for h in range(2)]
        return jnp.concatenate([jnp.concatenate(p, axis=1) for p in parts], axis=0)

    norms = []
    for c in range(NARROW):
        value = raw[c] * jnp.exp(-rate[place + c] * fraction)
        raw[c] = value
        norms.append(jnp.sqrt(total(value * value) + EPSILON))
    forward(lambda c: raw[c] / norms[c], spec_f, 0, NARROW)
    sgs[...] = jnp.zeros_like(sgs)

    def store_grad(c, y):
        y = y + gain[place + c] * blocks_of(c_recv, c, 16)
        for h in range(2):
            for q in range(2):
                y_send[pl.ds(4 * c + 2 * h + q, 64, stride=16), :] = y[h * 64 : h * 64 + 64, q * 128 : q * 128 + 128]

    if comm:
        landed(c_recv.at[pl.ds(0, (GROUPS - 1) * 16)], recv_sem, 0)
    forward(lambda c: blocks_of(c_recv, c, 16), spec_c, 0, NARROW)
    for pair in range(2):
        inverse(spec_f, 2 * pair, pair, lambda c, y: store_grad(2 * pair + c, y))
    if comm:
        spread(y_send, y_recv, 4, 16, 16, 0, 0, 16)
    else:
        for r in range(8):
            y_recv[r * 128 : r * 128 + 128, :] = y_send[r * 128 : r * 128 + 128, :]

    def filter_grad(pair):
        if comm:
            arrived(s_recv[pair], recv_sem, 2 + pair)
        forward(lambda c: blocks_of(s_recv[pair], c, 8), spec_s, 0, 2)

        def store(c, y):
            ch = 2 * pair + c
            dfilt = FACTOR * y
            norm = norms[ch]
            value = raw[ch]
            filt = value / norm
            project = total(filt * dfilt)
            draw = (dfilt - filt * project) / norm
            decay = -jnp.sum(draw * value * fraction, axis=0, keepdims=True)
            skip = blocks_of(c_recv, ch, 16) * blocks_of(s_recv[pair], c, 8)
            skip = FACTOR * jnp.sum(skip, axis=0, keepdims=True)
            sgs[ch * 128 + 64 : ch * 128 + 65, :] = decay[:, :128] + decay[:, 128:]
            sgs[ch * 128 + 65 : ch * 128 + 66, :] = skip[:, :128] + skip[:, 128:]
            dmix[ch] = draw * jnp.exp(-rate[place + ch] * fraction)

        inverse(spec_s, 0, pair, store)

    def half_back(step, _):
        for r in range(0, A, 16):
            rows = slice(r, r + 16)
            d = [dmix[c, rows, :] for c in range(2)]
            for i in range(KK):
                k = step * KK + i
                part[k, rows, :] = d[0] * cols[k, place] + d[1] * cols[k, place + 1]
        return 0

    def fill(buf, step):
        for r in range(0, A, 16):
            rows = slice(r, r + 16)
            d = [dmix[c, rows, :] for c in range(2, 4)]
            for i in range(KK):
                k = step * KK + i
                g = part[k, rows, :] + d[0] * cols[k, place + 2] + d[1] * cols[k, place + 3]
                ghi, glo = halves(g * cosb[k, rows, :])
                buf[i * A + r : i * A + r + 16, :M] = ghi
                buf[i * A + r : i * A + r + 16, M:] = glo

    def contract(buf, step):
        hmat = dot(buf[...], t["qb"][...])
        for i in range(KK):
            h = hmat[i * A : i * A + A]
            at = pl.ds(step * KK + i + 8, 1)
            ug[at, :] = jnp.sum(h * t["ca"][...], axis=0, keepdims=True)
            vg[at, :] = jnp.sum(h * t["sa"][...], axis=0, keepdims=True)

    def first_back(two, _):
        fill(gh, 2 * two)
        contract(gl, 2 * two - 1)
        fill(gl, 2 * two + 1)
        contract(gh, 2 * two)
        return 0

    def second_back(pair, step, _):
        sums = [[jnp.zeros((8, 128), F32) for _ in range(2)] for _ in range(KK)]
        for r in range(0, A, 16):
            rows = slice(r, r + 16)
            d = [dmix[2 * pair + c, rows, :] for c in range(2)]
            for i in range(KK):
                b = basis[step * KK + i, rows, :]
                for c in range(2):
                    e = b * d[c]
                    sums[i][c] = sums[i][c] + ((e[:8, :128] + e[:8, 128:]) + (e[8:, :128] + e[8:, 128:]))
        for i in range(KK):
            for c in range(2):
                at = (2 * pair + c) * 128 + step * KK + i
                sgs[pl.ds(at, 1), :] = jnp.sum(sums[i][c], axis=0, keepdims=True)
        return 0

    filter_grad(0)
    lax.fori_loop(0, ORDER // KK, half_back, 0)
    lax.fori_loop(0, ORDER // KK, functools.partial(second_back, 0), 0)
    filter_grad(1)
    lax.fori_loop(0, ORDER // KK // 2, first_back, 0)
    contract(gl, ORDER // KK - 1)

    across = (((1,), (1,)), ((), ()))
    hdot = lambda a, b: lax.dot_general(a, b, across, precision=high, preferred_element_type=F32)
    lanes = lax.broadcasted_iota(jnp.int32, (1, 128), 1)
    two = lambda x: jnp.where(lanes < 2 * TERMS, x, 0.0)
    picks = jnp.concatenate([two(t["ea"][...]), two(t["eb"][...])], axis=1).astype(BF16)
    rest = jnp.concatenate([ug[8:, :], vg[8:, :]], axis=1)
    first = jnp.zeros((40, ORDER), F32)
    for _ in range(3):
        piece = rest.astype(BF16)
        rest = rest - piece.astype(F32)
        first = first + lax.dot_general(picks, piece, across, preferred_element_type=F32)
    first = jnp.concatenate(
        [
            jnp.concatenate([first[:16], first[16:32]], axis=1),
            jnp.concatenate([first[32:33], jnp.zeros((1, 64), F32)], axis=1),
        ],
        axis=0,
    )

    def issue(buf, slot, value, me, count, target):
        buf[pl.ds(me, 1)] = value[None]
        for i in range(1, count):
            pltpu.make_async_remote_copy(
                src_ref=buf.at[me],
                dst_ref=buf.at[me],
                send_sem=send_sem.at[slot],
                recv_sem=recv_sem.at[slot],
                device_id=target(lax.rem(me + i, count)),
                device_id_type=MESH,
            ).start()

    def collect(buf, slot, count):
        landed(buf.at[pl.ds(0, count - 1)], recv_sem, slot)
        value = buf[0]
        for i in range(1, count):
            value = value + buf[i]
        return value

    zi, xi, yi, xy = bi // 8, lax.rem(bi // 2, 4), lax.rem(bi, 2), lax.rem(bi, 8)
    along_y = lambda p: {"batch": bi - yi + p // PEERS, "chan": lax.rem(p, PEERS)}
    along_x = lambda p: {"batch": zi * 8 + p * 2 + yi}
    along_z = lambda p: {"batch": p * 8 + xy}
    in_plane = lambda p: {"batch": zi * 8 + p}
    if comm:
        issue(red_a, 7, first, yi * PEERS + ci, 8, along_y)

    lax.fori_loop(0, ORDER // KK, functools.partial(second_back, 1), 0)
    ones = jnp.ones((8, 128), F32)
    block = jnp.concatenate([hdot(ones, sgs[c * 128 : c * 128 + 128, :])[:1] for c in range(NARROW)], axis=0)

    if not comm:
        gath[...] = jnp.zeros_like(gath)
        gath[0] = block
        first_out[...] = first
        return

    issue(gath_z, 5, block, zi, 8, along_z)
    first = collect(red_a, 7, 8)
    issue(red_c, 8, first, xi, 4, along_x)
    landed(gath_z.at[pl.ds(0, 7)], recv_sem, 5)
    issue(gath, 6, gath_z[...], xy, 8, in_plane)
    first = collect(red_c, 8, 4)
    issue(red_b, 9, first, zi, 8, along_z)

    whole = y_recv.at[pl.ds(0, (GROUPS - 1) * 16)]
    landed(whole, recv_sem, 4)
    for q in range(4):
        grad[:, q * 128 : q * 128 + 128] = y_recv[pl.ds(q, 256, stride=4), :]
    landed(gath.at[pl.ds(0, 7)], recv_sem, 6)
    every = jnp.concatenate([gath[:, z].reshape(8 * NARROW, 128) for z in range(8)], axis=0)
    turned = every.T
    second_grad[...] = turned[:ORDER]
    decay_grad[...] = turned[ORDER : ORDER + 1]
    skip_grad[...] = turned[ORDER + 1 : ORDER + 2]
    first = collect(red_b, 9, 8)
    first_grad[:16] = first[:16, :ORDER]
    first_grad[16:32] = first[:16, ORDER:]
    first_grad[32:33] = first[16:17, :ORDER]

    for slot in (0, 4):
        landed(whole, send_sem, slot)
    for slot in (2, 3):
        arrived(y_recv, send_sem, slot)
    landed(gath_z.at[pl.ds(0, 7)], send_sem, 5)
    landed(gath.at[pl.ds(0, 7)], send_sem, 6)
    landed(red_a.at[pl.ds(0, 7)], send_sem, 7)
    landed(red_c.at[pl.ds(0, 3)], send_sem, 8)
    landed(red_b.at[pl.ds(0, 7)], send_sem, 9)


def finish(*refs):
    sem = refs[10]
    copies = [pltpu.make_async_copy(refs[i], refs[5 + i], sem.at[i]) for i in range(5)]
    for copy in copies:
        copy.start()
    for copy in copies:
        copy.wait()


def call(comm, sig, cot, first_layer, second_layer, rate, gain):
    vmem = pl.BlockSpec(memory_space=pltpu.VMEM)
    anywhere = pl.BlockSpec(memory_space=pltpu.HBM)
    t = tables()
    line = lambda: pltpu.VMEM((GROUPS * 16, 128), F32)
    half = lambda: pltpu.VMEM((GROUPS * 8, 128), F32)
    scratch = [pltpu.VMEM(t[name].shape, t[name].dtype) for name in NAMES]
    scratch += [
        pltpu.VMEM(sig.shape, F32),
        pltpu.VMEM(cot.shape, F32),
        pltpu.VMEM(first_layer.shape, F32),
        pltpu.SMEM(second_layer.shape, F32),
        pltpu.SMEM(rate.shape, F32),
        pltpu.SMEM(gain.shape, F32),
        line(),
        line(),
    ]
    scratch += [half(), half(), line(), line()]
    scratch += [
        pltpu.VMEM((ORDER, A, M), F32),
        pltpu.VMEM((ORDER, A, M), F32),
        pltpu.VMEM((ORDER, A, M), F32),
        pltpu.VMEM((KK * A, 128), BF16),
        pltpu.VMEM((KK * A, M), F32),
        pltpu.VMEM((NARROW, A, M), F32),
        pltpu.VMEM((NARROW, A, M), F32),
        pltpu.VMEM((A, M), BF16),
        pltpu.VMEM((A, M), BF16),
        pltpu.VMEM((NARROW * A, 2 * M), BF16),
        pltpu.VMEM((NARROW * A, 2 * M), BF16),
        pltpu.VMEM((NARROW * A, 2 * M), F32),
        pltpu.VMEM((NARROW * A, 2 * M), F32),
        pltpu.VMEM((2 * A, 2 * M), F32),
        pltpu.VMEM((2 * A, 2 * M), F32),
        pltpu.VMEM((2 * A, M), F32),
        pltpu.VMEM((NARROW * 128, 128), F32),
        pltpu.VMEM((ORDER, 128), F32),
        pltpu.VMEM((ORDER, 128), F32),
        pltpu.VMEM((ORDER + 8, 128), F32),
        pltpu.VMEM((ORDER + 8, 128), F32),
        pltpu.VMEM((8, 17, 128), F32),
        pltpu.VMEM((8, 17, 128), F32),
        pltpu.VMEM((4, 17, 128), F32),
        pltpu.SemaphoreType.DMA((10,)),
        pltpu.SemaphoreType.DMA((10,)),
        pltpu.SemaphoreType.DMA((6 + len(NAMES),)),
    ]
    params = dict(vmem_limit_bytes=VMEM_LIMIT)
    shapes = out_shapes(sig, first_layer, second_layer, rate, gain)
    if comm:
        scratch += [line(), pltpu.VMEM((8, NARROW, 128), F32), pltpu.VMEM((8, 8, NARROW, 128), F32)]
        params.update(collective_id=0, has_side_effects=True)
    return pl.pallas_call(
        functools.partial(kernel, comm),
        out_shape=tuple(OUT(shape, F32) for shape in shapes) if comm else tuple(
            jax.ShapeDtypeStruct(shape, F32) for shape in ((GROUPS * 16, 128), (GROUPS, NARROW, 128), (17, 128))
        ),
        in_specs=[anywhere] * (6 + len(NAMES)),
        out_specs=(vmem,) * (5 if comm else 3),
        scratch_shapes=scratch,
        compiler_params=pltpu.CompilerParams(**params),
        name="hyena_back",
    )(sig, cot, first_layer, second_layer, rate, gain, *[jnp.asarray(t[name]) for name in NAMES])


def out_shapes(sig, first_layer, second_layer, rate, gain):
    return sig.shape, first_layer.shape, second_layer.shape, (1, rate.shape[0]), (1, gain.shape[0])


def local(signal, cotangent, first_layer, second_layer, decay_rate, skip_gain):
    held = call(True, signal, cotangent, first_layer, second_layer, decay_rate, skip_gain)
    shapes = out_shapes(signal, first_layer, second_layer, decay_rate, skip_gain)
    grad, first_grad, second_grad, decay_grad, skip_grad = pl.pallas_call(
        finish,
        out_shape=tuple(jax.ShapeDtypeStruct(shape, F32) for shape in shapes),
        in_specs=[pl.BlockSpec(memory_space=pltpu.VMEM if PIN else pl.ANY)] * 5,
        out_specs=(pl.BlockSpec(memory_space=pl.ANY),) * 5,
        scratch_shapes=[pltpu.SemaphoreType.DMA((5,))],
        compiler_params=pltpu.CompilerParams(vmem_limit_bytes=4 * 2**20),
        name="finish",
    )(*held)
    return grad, first_grad, second_grad, decay_grad.reshape(-1), skip_grad.reshape(-1)


def solution(mesh):
    placed = (P("chan", "batch"), P("chan", "batch"), P(), P(None, "chan"), P("chan"), P("chan"))
    return jax.shard_map(
        local,
        mesh=mesh,
        in_specs=placed,
        out_specs=(P("chan", "batch"), P(), P(None, "chan"), P("chan"), P("chan")),
        check_vma=False,
    )
```
